256 devices in a mesh: grp: 32 (over z, x), tp: 8 (over y, core).
Axes of the slice: x: 4, y: 4, z: 8, core: 2. Of those that a mesh axis runs over, the one named last changes fastest.
Arguments:
- suffix_cache: bfloat16 [128, 512, 2, 1024], P('grp', None, None, 'tp'), may hold values from -6 to 6
- prompt_cache: bfloat16 [64, 512, 2, 1024], P('grp', None, None, 'tp'), may hold values from -6 to 6
- query_first: bfloat16 [128, 8192], P('grp', 'tp'), may hold values from -45 to 45
- fresh_first: bfloat16 [128, 2, 1024], P('grp', None, 'tp'), may hold values from -6 to 6
- query_second: bfloat16 [128, 8192], P('grp', 'tp'), may hold values from -45 to 45
- fresh_second: bfloat16 [128, 2, 1024], P('grp', None, 'tp'), may hold values from -6 to 6
- out_weight: bfloat16 [8192, 4096], P('tp'), may hold values from -1 to 1
- suffix_len: int32 [128], replicated, may hold values from 0 to 511, as said below
- prompt_slot: int32 [128], P('grp'), may hold values from -1 to 1, as said below
- moves: int32 [8, 5], replicated, may hold values from 0 to 31, as said below
Outputs:
- out_first: bfloat16 [128, 4096], P('grp', 'tp')
- out_second: bfloat16 [128, 4096], P('grp', 'tp')
The draws below stay inside these ranges and needn't reach their ends.
Inputs may be any that keep to these rules, and one draw needn't show every extreme that they name: `suffix_len`: 0 exactly on empty slots, 1 or more on live ones. Every group has exactly one empty slot before the migration. The source of every move is live and its length is 384 or more; some source has 511. `prompt_slot`: each group's live samples read its prompt slots; in every destination group all live samples read one prompt slot and the other is free. `moves`: source groups are distinct, destination groups are distinct, and no group is both. The destination slot is the destination group's empty slot and the destination prompt slot is its free prompt slot.
All inputs are finite; a program needn't handle non-finite values.
Results may differ from the reference program's by a relative error of at most 0.0058.
Values may be sent and summed in bfloat16 or wider, within the bound.
No kernel may reach another device: no remote copies, remote signals or barrier semaphores. Data moves between devices by JAX's collectives and lax.ppermute only.
A program may use at most 128 MiB of HBM per device.

```python
import jax
import jax.numpy as jnp
from jax import lax

QH = 64
KVH = 8
HD = 128
DOUT = 4096
SLOTS = 4
SUF = 512
PROMPT = 512
PSLOTS = 2
N_GRP_SAMPLES = 128
MOVES = 8
N_GRP = 32


def layout_tables(key):
    streams = jax.random.split(jax.random.fold_in(key, 7), 9)
    half = N_GRP // 2
    residues = jax.random.permutation(streams[0], half)[:MOVES]
    upper = jax.random.randint(streams[7], (MOVES,), 0, 2)
    sources = residues + upper * half
    partners = residues + (1 - upper) * half
    odd_count = MOVES // 2
    odd_order = jax.random.permutation(streams[8], odd_count)
    mapping = jnp.arange(MOVES).at[2 * jnp.arange(odd_count) + 1].set(2 * odd_order + 1)
    targets = partners[mapping]
    empty_slot = jax.random.randint(streams[1], (N_GRP,), 0, SLOTS)
    source_slot = (empty_slot[sources] + 1 + jax.random.randint(streams[2], (MOVES,), 0, SLOTS - 1)) % SLOTS
    target_slot = empty_slot[targets]
    free_prompt = jax.random.randint(streams[3], (N_GRP,), 0, 2)
    target_prompt = free_prompt[targets]
    is_target = jnp.zeros((N_GRP,), jnp.int32).at[targets].set(1)
    usage = jax.random.randint(streams[4], (N_GRP, SLOTS), 0, 2)
    usage = jnp.where(is_target[:, None] == 1, 1 - free_prompt[:, None], usage)
    slot_ids = jnp.arange(SLOTS)[None, :]
    prompt_ids = jnp.where(slot_ids == empty_slot[:, None], -1, usage)
    lengths = jax.random.randint(streams[5], (N_GRP, SLOTS), 1, SUF)
    long_lengths = jax.random.randint(streams[6], (MOVES,), 3 * SUF // 4, SUF)
    long_lengths = long_lengths.at[0].set(SUF - 1)
    lengths = lengths.at[sources, source_slot].set(long_lengths)
    lengths = jnp.where(slot_ids == empty_slot[:, None], 0, lengths)
    move_rows = jnp.stack([sources, source_slot, targets, target_slot, target_prompt], 1).astype(jnp.int32)
    return (lengths.reshape(-1).astype(jnp.int32), prompt_ids.reshape(-1).astype(jnp.int32), move_rows)


def float_draws(key):
    streams = jax.random.split(jax.random.fold_in(key, 23), 3)
    prompt_shape = (N_GRP * PSLOTS, PROMPT, 2, KVH * HD)
    query_shape = (N_GRP * SLOTS, QH * HD)
    prompt = jnp.clip(jax.random.normal(streams[0], prompt_shape, jnp.float32), -6.0, 6.0)
    first = jnp.clip(jax.random.normal(streams[1], query_shape, jnp.float32), -6.0, 6.0)
    second = jnp.clip(jax.random.normal(streams[2], query_shape, jnp.float32), -6.0, 6.0)
    return (prompt, first, second)


def draw_prompt_cache(key, part):
    return float_draws(key)[0].astype(jnp.bfloat16)


def draw_query_first(key, part):
    return float_draws(key)[1].astype(jnp.bfloat16)


def draw_query_second(key, part):
    return float_draws(key)[2].astype(jnp.bfloat16)


def draw_suffix_len(key, part):
    return layout_tables(key)[0]


def draw_prompt_slot(key, part):
    return layout_tables(key)[1]


def draw_moves(key, part):
    return layout_tables(key)[2]


def levels(own_key, dims, cuts, least, largest):
    gain, own = 1.0, jax.random.fold_in(own_key, 6)
    for position, parts in cuts:
        draws = jnp.exp(jax.random.uniform(jax.random.fold_in(own, position), (parts,), jnp.float32, least / len(cuts), largest / len(cuts)))
        gain = gain * jnp.repeat(draws, dims[position] // parts).reshape([-1 if axis == position else 1 for axis in range(len(dims))])
    return gain


def bell_draw(key, extent, deviation, most, cuts=(), held_as=jnp.bfloat16):
    loudness = levels(key, extent, cuts, -0.22, 0.18) if cuts else 1.0
    array = jax.random.normal(key, extent, jnp.float32) * deviation * loudness
    return jnp.minimum(jnp.maximum(array, -most), most).astype(held_as)


def setup_inputs(seed: int = 0) -> dict:
    arg_keys = jax.random.split(jax.random.key(seed), 11)
    return {
        "suffix_cache": bell_draw(arg_keys[0], (N_GRP_SAMPLES, SUF, 2, KVH * HD), 1.0, 6.0, ((0, 32), (3, 8))),
        "prompt_cache": draw_prompt_cache(jax.random.fold_in(arg_keys[10], 71), 0),
        "query_first": draw_query_first(jax.random.fold_in(arg_keys[10], 71), 0),
        "fresh_first": bell_draw(arg_keys[3], (N_GRP_SAMPLES, 2, KVH * HD), 1.0, 6.0, ((0, 32), (2, 8))),
        "query_second": draw_query_second(jax.random.fold_in(arg_keys[10], 71), 0),
        "fresh_second": bell_draw(arg_keys[5], (N_GRP_SAMPLES, 2, KVH * HD), 1.0, 6.0, ((0, 32), (2, 8))),
        "out_weight": bell_draw(arg_keys[6], (QH * HD, DOUT), (HD // 4) ** -0.5, 1.0, ((0, 8),)),
        "suffix_len": draw_suffix_len(jax.random.fold_in(arg_keys[10], 71), 0),
        "prompt_slot": draw_prompt_slot(jax.random.fold_in(arg_keys[10], 71), 0),
        "moves": draw_moves(jax.random.fold_in(arg_keys[10], 71), 0),
    }


def attend_sample(queries, prompt_kv, suffix_kv, fresh, length):
    key_rows = jnp.concatenate([prompt_kv[:, 0], suffix_kv[:, 0], fresh[None, 0]], 0).astype(jnp.float32)
    value_rows = jnp.concatenate([prompt_kv[:, 1], suffix_kv[:, 1], fresh[None, 1]], 0).astype(jnp.float32)
    total_rows = key_rows.shape[0]
    key_rows = key_rows.reshape(total_rows, KVH, HD)
    value_rows = value_rows.reshape(total_rows, KVH, HD)
    heads = queries.astype(jnp.float32).reshape(KVH, QH // KVH, HD)
    scores = jnp.einsum("kgd,lkd->kgl", heads, key_rows) * (HD ** -0.5)
    valid = jnp.concatenate([jnp.ones((PROMPT,), bool), jnp.arange(SUF, dtype=jnp.int32) < length, jnp.ones((1,), bool)])
    scores = jnp.where(valid[None, None, :], scores, -1e30)
    highest = jnp.max(scores, -1, keepdims=True)
    spread = jnp.exp(scores - highest)
    weights = (spread / jnp.sum(spread, -1, keepdims=True)).astype(jnp.bfloat16)
    weights = lax.optimization_barrier(weights).astype(jnp.float32)
    mixed = jnp.einsum("kgl,lkd->kgd", weights, value_rows)
    return mixed.reshape(QH * HD)


def decode_all(queries, prompt_cache, suffix_cache, fresh, lengths, prompt_ids):
    def one_sample(sample):
        prompt_row = (sample // SLOTS) * PSLOTS + jnp.maximum(prompt_ids[sample], 0)
        result = attend_sample(queries[sample], prompt_cache[prompt_row], suffix_cache[sample], fresh[sample], lengths[sample])
        return jnp.where(prompt_ids[sample] >= 0, result, 0.0).astype(jnp.bfloat16)

    return lax.map(one_sample, jnp.arange(queries.shape[0], dtype=jnp.int32))


def reference(suffix_cache, prompt_cache, query_first, fresh_first, query_second, fresh_second, out_weight, suffix_len, prompt_slot, moves):
    attn_first = decode_all(query_first, prompt_cache, suffix_cache, fresh_first, suffix_len, prompt_slot)
    positions = jnp.arange(SUF, dtype=jnp.int32)
    write_mask = (positions[None, :] == suffix_len[:, None]) & (prompt_slot[:, None] >= 0)
    appended = jnp.where(write_mask[:, :, None, None], fresh_first[:, None], suffix_cache)
    source_rows = (moves[:, 0] * SLOTS + moves[:, 1]).astype(jnp.int32)
    target_rows = (moves[:, 2] * SLOTS + moves[:, 3]).astype(jnp.int32)
    prompt_from = (moves[:, 0] * PSLOTS + prompt_slot[source_rows]).astype(jnp.int32)
    prompt_into = (moves[:, 2] * PSLOTS + moves[:, 4]).astype(jnp.int32)
    suffix_moved = appended.at[target_rows].set(appended[source_rows])
    prompt_moved = prompt_cache.at[prompt_into].set(prompt_cache[prompt_from])
    grown = jnp.where(prompt_slot >= 0, suffix_len + 1, 0).astype(jnp.int32)
    length_moved = grown.at[target_rows].set(grown[source_rows]).at[source_rows].set(0)
    slot_moved = prompt_slot.at[target_rows].set(moves[:, 4]).at[source_rows].set(-1)
    attn_second = decode_all(query_second, prompt_moved, suffix_moved, fresh_second, length_moved, slot_moved)
    out_first = jnp.dot(attn_first, out_weight, preferred_element_type=jnp.float32).astype(jnp.bfloat16)
    out_second = jnp.dot(attn_second, out_weight, preferred_element_type=jnp.float32).astype(jnp.bfloat16)
    return out_first, out_second
```

```python
import jax
import jax.numpy as jnp
from jax import lax
from jax.experimental import pallas as pl
from jax.experimental.pallas import tpu as pltpu
from jax.sharding import PartitionSpec as P

QH = 64
KVH = 8
HD = 128
HEADS = QH // KVH

BF = jnp.bfloat16
F32 = jnp.float32
SMEM = pl.BlockSpec(memory_space=pltpu.SMEM)
VMEM = pl.BlockSpec(memory_space=pltpu.VMEM)


def empty_slot_of(slot_ref):
    found = jnp.int32(0)
    for s in range(slot_ref.shape[0]):
        found = jnp.where(slot_ref[s] < 0, jnp.int32(s), found)
    return found


def look_up(moves_ref, own, key, fields):
    hit_any = jnp.int32(0)
    values = [jnp.int32(0) for _ in fields]
    for i in range(moves_ref.shape[0]):
        hit = moves_ref[i, key] == own
        hit_any = jnp.where(hit, jnp.int32(1), hit_any)
        values = [jnp.where(hit, moves_ref[i, f], v) for f, v in zip(fields, values)]
    return hit_any, values


def offer_kernel(slot_ref, query_ref, fresh_ref, out_ref):
    empty = empty_slot_of(slot_ref)
    slots = query_ref.shape[0]
    mine = lax.broadcasted_iota(jnp.int32, (slots, HD), 0) == empty
    rows = []
    for h in range(HEADS):
        part = query_ref[:, h * HD : (h + 1) * HD].astype(F32)
        rows.append(jnp.sum(jnp.where(mine, part, 0.0), axis=0, keepdims=True))
    pair = jnp.zeros((2, HD), F32)
    for s in range(slots):
        pair = jnp.where(empty == s, fresh_ref[s].astype(F32), pair)
    rows += [pair, jnp.zeros((6, HD), F32)]
    block = jnp.concatenate(rows, axis=0).astype(BF)
    out_ref[...] = jnp.broadcast_to(block[None], out_ref.shape)


def attend_kernel(
    own_ref,
    len_ref,
    slot_ref,
    moves_ref,
    query_first_ref,
    query_second_ref,
    fresh_first_ref,
    fresh_second_ref,
    offers_ref,
    prompt_ref,
    suffix_ref,
    rows_ref,
    moved_ref,
    queries_ref,
):
    own = own_ref[0]
    slots = query_first_ref.shape[0]
    prompt_width = prompt_ref.shape[1]
    suffix_width = suffix_ref.shape[1]
    is_source, (out_slot, destination) = look_up(moves_ref, own, 0, (1, 2))
    for h in range(HEADS):
        queries_ref[:, h, :] = query_first_ref[:, h * HD : (h + 1) * HD].astype(F32)
        queries_ref[:, HEADS + h, :] = query_second_ref[:, h * HD : (h + 1) * HD].astype(F32)
    offer = offers_ref[destination].astype(F32)
    scale = HD ** (-0.5)
    second_row = lax.broadcasted_iota(jnp.int32, (2 * HEADS, 1), 0) >= HEADS
    prompt_keys = lax.broadcasted_iota(jnp.int32, (2 * HEADS, prompt_width), 1) % 2 == 0
    column = lax.broadcasted_iota(jnp.int32, (2 * HEADS, suffix_width), 1)
    suffix_keys = column % 2 == 0
    moved = jnp.zeros((HEADS, HD), F32)
    contract_last = (((1,), (1,)), ((), ()))
    for s in range(slots):
        leaving = (is_source == 1) & (out_slot == s)
        length = len_ref[own * slots + s]
        prompt_id = slot_ref[s]
        live = prompt_id >= 0
        first = queries_ref[s, :HEADS, :]
        second = jnp.where(leaving, offer[:HEADS], queries_ref[s, HEADS:, :])
        both = jnp.concatenate([first, second], axis=0)
        pair_first = fresh_first_ref[s].astype(F32)
        pair_second = jnp.where(leaving, offer[HEADS : HEADS + 2], fresh_second_ref[s].astype(F32))
        queries = both.astype(BF)
        prompt = prompt_ref[jnp.maximum(prompt_id, 0)]
        suffix = suffix_ref[s]
        on_prompt = (
            lax.dot_general(queries, prompt, contract_last, preferred_element_type=F32) * scale
        )
        on_suffix = (
            lax.dot_general(queries, suffix, contract_last, preferred_element_type=F32) * scale
        )
        on_prompt = jnp.where(prompt_keys, on_prompt, -1e30)
        on_suffix = jnp.where(suffix_keys & (column < 2 * length), on_suffix, -1e30)
        on_first = jnp.sum(both * pair_first[0:1], axis=1, keepdims=True) * scale
        on_second = jnp.sum(both * pair_second[0:1], axis=1, keepdims=True) * scale
        on_second = jnp.where(second_row, on_second, -1e30)
        highest = jnp.maximum(
            jnp.max(on_prompt, axis=1, keepdims=True), jnp.max(on_suffix, axis=1, keepdims=True)
        )
        highest = jnp.maximum(highest, jnp.maximum(on_first, on_second))
        prompt_spread = jnp.exp(on_prompt - highest)
        suffix_spread = jnp.exp(on_suffix - highest)
        first_spread = jnp.exp(on_first - highest)
        second_spread = jnp.exp(on_second - highest)
        total = (
            jnp.sum(prompt_spread, axis=1, keepdims=True)
            + jnp.sum(suffix_spread, axis=1, keepdims=True)
            + first_spread
            + second_spread
        )
        share = 1.0 / total
        prompt_weights = pltpu.roll(prompt_spread * share, 1, 1).astype(BF)
        suffix_weights = pltpu.roll(suffix_spread * share, 1, 1).astype(BF)
        mixed = lax.dot(prompt_weights, prompt, preferred_element_type=F32)
        mixed += lax.dot(suffix_weights, suffix, preferred_element_type=F32)
        mixed += (first_spread * share).astype(BF).astype(F32) * pair_first[1:2]
        mixed += (second_spread * share).astype(BF).astype(F32) * pair_second[1:2]
        mixed = mixed.astype(BF).astype(F32)
        stays = live & jnp.logical_not(leaving)
        rows_ref[:, s, :] = jnp.where(live, mixed[:HEADS], 0.0)
        rows_ref[:, slots + s, :] = jnp.where(stays, mixed[HEADS:], 0.0)
        moved = jnp.where(leaving, mixed[HEADS:], moved)
    moved_ref[...] = jnp.broadcast_to(moved.astype(BF)[None], moved_ref.shape)


def project_kernel(own_ref, slot_ref, moves_ref, rows_ref, arrived_ref, weight_ref, out_ref):
    own = own_ref[0]
    slots = slot_ref.shape[0]
    is_target, (in_source,) = look_up(moves_ref, own, 2, (0,))
    row = jnp.where(is_target == 1, slots + empty_slot_of(slot_ref), -1)
    arrived = arrived_ref[in_source].astype(F32)
    into = lax.broadcasted_iota(jnp.int32, (2 * slots, HD), 0) == row
    parts = [jnp.where(into, arrived[h : h + 1], rows_ref[h]) for h in range(HEADS)]
    rows = jnp.concatenate(parts, axis=1).astype(BF)
    width = out_ref.shape[2]
    for t in range(out_ref.shape[0]):
        out_ref[t] = lax.dot(
            rows, weight_ref[:, t * width : (t + 1) * width], preferred_element_type=F32
        )


def sum_kernel(parts_ref, first_ref, second_ref):
    total = jnp.sum(parts_ref[...], axis=0)
    slots = first_ref.shape[0]
    first_ref[...] = total[:slots].astype(BF)
    second_ref[...] = total[slots:].astype(BF)


def per_device(
    suffix_cache,
    prompt_cache,
    query_first,
    fresh_first,
    query_second,
    fresh_second,
    out_weight,
    suffix_len,
    prompt_slot,
    moves,
):
    slots, cap = suffix_cache.shape[:2]
    prompts, prompt_len = prompt_cache.shape[:2]
    groups = lax.axis_size("grp")
    shares = lax.axis_size("tp")
    features = out_weight.shape[1]
    own = lax.axis_index("grp").astype(jnp.int32).reshape(1)
    suffix_rows = suffix_cache.reshape(slots, 2 * cap, HD)
    prompt_rows = prompt_cache.reshape(prompts, 2 * prompt_len, HD)
    offer = pl.pallas_call(
        offer_kernel,
        out_shape=jax.ShapeDtypeStruct((groups, 2 * HEADS, HD), BF),
        in_specs=[SMEM, VMEM, VMEM],
        out_specs=VMEM,
        name="offer",
    )(prompt_slot, query_second, fresh_second)
    offers = lax.all_to_all(offer, "grp", 0, 0, tiled=True)
    rows, moved = pl.pallas_call(
        attend_kernel,
        out_shape=(
            jax.ShapeDtypeStruct((HEADS, 2 * slots, HD), F32),
            jax.ShapeDtypeStruct((groups, HEADS, HD), BF),
        ),
        in_specs=[SMEM, SMEM, SMEM, SMEM] + [VMEM] * 7,
        out_specs=(VMEM, VMEM),
        scratch_shapes=[pltpu.VMEM((slots, 2 * HEADS, HD), F32)],
        name="attend",
    )(
        own,
        suffix_len,
        prompt_slot,
        moves,
        query_first,
        query_second,
        fresh_first,
        fresh_second,
        offers,
        prompt_rows,
        suffix_rows,
    )
    arrived = lax.all_to_all(moved, "grp", 0, 0, tiled=True)
    parts = pl.pallas_call(
        project_kernel,
        out_shape=jax.ShapeDtypeStruct((shares, 2 * slots, features // shares), F32),
        in_specs=[SMEM, SMEM, SMEM, VMEM, VMEM, VMEM],
        out_specs=VMEM,
        name="project",
    )(own, prompt_slot, moves, rows, arrived, out_weight)
    parts = lax.all_to_all(parts, "tp", 0, 0, tiled=True)
    out = jax.ShapeDtypeStruct((slots, features // shares), BF)
    return pl.pallas_call(
        sum_kernel,
        out_shape=(out, out),
        in_specs=[VMEM],
        out_specs=(VMEM, VMEM),
        name="sum",
    )(parts)


def solution(mesh):
    placed = (
        P("grp", None, None, "tp"),
        P("grp", None, None, "tp"),
        P("grp", "tp"),
        P("grp", None, "tp"),
        P("grp", "tp"),
        P("grp", None, "tp"),
        P("tp", None),
        P(),
        P("grp"),
        P(),
    )
    return jax.shard_map(
        per_device,
        mesh=mesh,
        in_specs=placed,
        out_specs=(P("grp", "tp"), P("grp", "tp")),
        check_vma=False,
    )
```

```python
import jax
import jax.numpy as jnp
from jax import lax
from jax.experimental import pallas as pl
from jax.experimental.pallas import tpu as pltpu
from jax.sharding import PartitionSpec as P

QH = 64
KVH = 8
HD = 128
HEADS = QH // KVH

BF = jnp.bfloat16
F32 = jnp.float32
SMEM = pl.BlockSpec(memory_space=pltpu.SMEM)
VMEM = pl.BlockSpec(memory_space=pltpu.VMEM)


SMALL = pltpu.CompilerParams(vmem_limit_bytes=8 << 20)


def near(array):
    return pltpu.with_memory_space_constraint(array, pltpu.VMEM)


def empty_slot_of(slot_ref):
    found = jnp.int32(0)
    for s in range(slot_ref.shape[0]):
        found = jnp.where(slot_ref[s] < 0, jnp.int32(s), found)
    return found


def look_up(moves_ref, own, key, fields):
    hit_any = jnp.int32(0)
    values = [jnp.int32(0) for _ in fields]
    for i in range(moves_ref.shape[0]):
        hit = moves_ref[i, key] == own
        hit_any = jnp.where(hit, jnp.int32(1), hit_any)
        values = [jnp.where(hit, moves_ref[i, f], v) for f, v in zip(fields, values)]
    return hit_any, values


def offer_kernel(slot_ref, query_ref, fresh_ref, out_ref):
    empty = empty_slot_of(slot_ref)
    slots = query_ref.shape[0]
    mine = lax.broadcasted_iota(jnp.int32, (slots, HD), 0) == empty
    rows = []
    for h in range(HEADS):
        part = query_ref[:, h * HD : (h + 1) * HD].astype(F32)
        rows.append(jnp.sum(jnp.where(mine, part, 0.0), axis=0, keepdims=True))
    pair = jnp.zeros((2, HD), F32)
    for s in range(slots):
        pair = jnp.where(empty == s, fresh_ref[s].astype(F32), pair)
    rows += [pair, jnp.zeros((6, HD), F32)]
    block = jnp.concatenate(rows, axis=0).astype(BF)
    out_ref[...] = jnp.broadcast_to(block[None], out_ref.shape)


def attend(queries, cached, pairs):
    scale = HD ** (-0.5)
    narrow = queries.astype(BF)
    row = lax.broadcasted_iota(jnp.int32, (queries.shape[0], 1), 0)
    scores = []
    for rows, width in cached:
        score = (
            lax.dot_general(
                narrow, rows, (((1,), (1,)), ((), ())), preferred_element_type=F32
            )
            * scale
        )
        column = lax.broadcasted_iota(jnp.int32, score.shape, 1)
        counts = column % 2 == 0
        if width is not None:
            counts = counts & (column < width)
        scores.append(jnp.where(counts, score, -1e30))
    singles = []
    for pair, since in pairs:
        score = jnp.sum(queries * pair[0:1], axis=1, keepdims=True) * scale
        singles.append(jnp.where(row >= since, score, -1e30) if since else score)
    highest = singles[0]
    for score in singles[1:]:
        highest = jnp.maximum(highest, score)
    for score in scores:
        highest = jnp.maximum(highest, jnp.max(score, axis=1, keepdims=True))
    spreads = [jnp.exp(score - highest) for score in scores]
    single_spreads = [jnp.exp(score - highest) for score in singles]
    total = sum(single_spreads)
    for spread in spreads:
        total = total + jnp.sum(spread, axis=1, keepdims=True)
    share = 1.0 / total
    mixed = jnp.zeros(queries.shape, F32)
    for (rows, _), spread in zip(cached, spreads):
        weights = pltpu.roll(spread * share, 1, 1).astype(BF)
        mixed += lax.dot(weights, rows, preferred_element_type=F32)
    for (pair, _), spread in zip(pairs, single_spreads):
        mixed += (spread * share).astype(BF).astype(F32) * pair[1:2]
    return mixed.astype(BF)


def stay_kernel(
    own_ref,
    len_ref,
    slot_ref,
    moves_ref,
    query_first_ref,
    query_second_ref,
    fresh_first_ref,
    fresh_second_ref,
    prompt_ref,
    suffix_ref,
    rows_ref,
    kept_ref,
    pair_ref,
    facts_ref,
    queries_ref,
):
    own = own_ref[0]
    slots = query_first_ref.shape[0]
    is_source, (out_slot, destination) = look_up(moves_ref, own, 0, (1, 2))
    is_target, (in_source,) = look_up(moves_ref, own, 2, (0,))
    facts_ref[0] = destination
    facts_ref[1] = 2 * len_ref[own * slots + out_slot]
    facts_ref[2] = in_source
    facts_ref[3] = jnp.where(is_target == 1, slots + empty_slot_of(slot_ref), -1)
    for h in range(HEADS):
        queries_ref[:, h, :] = query_first_ref[:, h * HD : (h + 1) * HD].astype(F32)
        queries_ref[:, HEADS + h, :] = query_second_ref[:, h * HD : (h + 1) * HD].astype(F32)
    half = prompt_ref.shape[1]
    kept_ref[:half] = prompt_ref[jnp.maximum(slot_ref[out_slot], 0)]
    kept_ref[half:] = suffix_ref[out_slot]
    pair_ref[...] = fresh_first_ref[out_slot].astype(F32)
    for s in range(slots):
        prompt_id = slot_ref[s]
        live = prompt_id >= 0
        stays = live & jnp.logical_not((is_source == 1) & (out_slot == s))
        mixed = attend(
            queries_ref[s],
            (
                (prompt_ref[jnp.maximum(prompt_id, 0)], None),
                (suffix_ref[s], 2 * len_ref[own * slots + s]),
            ),
            ((fresh_first_ref[s].astype(F32), 0), (fresh_second_ref[s].astype(F32), HEADS)),
        ).astype(F32)
        rows_ref[:, s, :] = jnp.where(live, mixed[:HEADS], 0.0)
        rows_ref[:, slots + s, :] = jnp.where(stays, mixed[HEADS:], 0.0)


def leave_kernel(facts_ref, offers_ref, kept_ref, pair_ref, moved_ref):
    offer = offers_ref[facts_ref[0]].astype(F32)
    half = kept_ref.shape[0] // 2
    mixed = attend(
        offer[:HEADS],
        ((kept_ref[:half], None), (kept_ref[half:], facts_ref[1])),
        ((pair_ref[...], 0), (offer[HEADS : HEADS + 2], 0)),
    )
    moved_ref[...] = jnp.broadcast_to(mixed[None], moved_ref.shape)


def merge_kernel(facts_ref, rows_ref, arrived_ref, out_ref):
    arrived = arrived_ref[facts_ref[2]].astype(F32)
    into = lax.broadcasted_iota(jnp.int32, rows_ref.shape[1:], 0) == facts_ref[3]
    for h in range(HEADS):
        row = jnp.where(into, arrived[h : h + 1], rows_ref[h])
        out_ref[:, h * HD : (h + 1) * HD] = row.astype(BF)


def sum_kernel(parts_ref, first_ref, second_ref):
    total = jnp.sum(parts_ref[...], axis=0)
    slots = first_ref.shape[0]
    first_ref[...] = total[:slots].astype(BF)
    second_ref[...] = total[slots:].astype(BF)


def per_device(
    suffix_cache,
    prompt_cache,
    query_first,
    fresh_first,
    query_second,
    fresh_second,
    out_weight,
    suffix_len,
    prompt_slot,
    moves,
):
    slots, cap = suffix_cache.shape[:2]
    prompts, prompt_len = prompt_cache.shape[:2]
    groups = lax.axis_size("grp")
    shares = lax.axis_size("tp")
    features = out_weight.shape[1]
    own = lax.axis_index("grp").astype(jnp.int32).reshape(1)
    suffix_rows = suffix_cache.reshape(slots, 2 * cap, HD)
    prompt_rows = prompt_cache.reshape(prompts, 2 * prompt_len, HD)
    offer = pl.pallas_call(
        offer_kernel,
        out_shape=pltpu.VMEM((groups, 2 * HEADS, HD), BF),
        in_specs=[SMEM, VMEM, VMEM],
        out_specs=VMEM,
        name="offer",
    )(prompt_slot, query_second, fresh_second)
    offers = lax.all_to_all(offer, "grp", 0, 0, tiled=True)
    rows, kept, pair, facts = pl.pallas_call(
        stay_kernel,
        out_shape=(
            pltpu.VMEM((HEADS, 2 * slots, HD), F32),
            pltpu.VMEM((2 * cap + 2 * prompt_len, HD), BF),
            pltpu.VMEM((2, HD), F32),
            jax.ShapeDtypeStruct((4,), jnp.int32),
        ),
        in_specs=[SMEM] * 4 + [VMEM] * 6,
        out_specs=(VMEM, VMEM, VMEM, SMEM),
        scratch_shapes=[pltpu.VMEM((slots, 2 * HEADS, HD), F32)],
        name="stay",
    )(
        own,
        suffix_len,
        prompt_slot,
        moves,
        query_first,
        query_second,
        fresh_first,
        fresh_second,
        prompt_rows,
        suffix_rows,
    )
    moved = pl.pallas_call(
        leave_kernel,
        out_shape=pltpu.VMEM((groups, HEADS, HD), BF),
        in_specs=[SMEM, VMEM, VMEM, VMEM],
        out_specs=VMEM,
        compiler_params=SMALL,
        name="leave",
    )(facts, near(offers), near(kept), near(pair))
    arrived = lax.all_to_all(moved, "grp", 0, 0, tiled=True)
    merged = pl.pallas_call(
        merge_kernel,
        out_shape=pltpu.VMEM((2 * slots, HEADS * HD), BF),
        in_specs=[SMEM, VMEM, VMEM],
        out_specs=VMEM,
        compiler_params=SMALL,
        name="merge",
    )(facts, near(rows), near(arrived))
    parts = jnp.dot(merged, out_weight, preferred_element_type=F32)
    parts = parts.reshape(2 * slots, shares, features // shares).swapaxes(0, 1)
    parts = lax.all_to_all(parts, "tp", 0, 0, tiled=True)
    out = jax.ShapeDtypeStruct((slots, features // shares), BF)
    return pl.pallas_call(
        sum_kernel,
        out_shape=(out, out),
        in_specs=[VMEM],
        out_specs=(VMEM, VMEM),
        compiler_params=SMALL,
        name="sum",
    )(near(parts))


def solution(mesh):
    placed = (
        P("grp", None, None, "tp"),
        P("grp", None, None, "tp"),
        P("grp", "tp"),
        P("grp", None, "tp"),
        P("grp", "tp"),
        P("grp", None, "tp"),
        P("tp", None),
        P(),
        P("grp"),
        P(),
    )
    return jax.shard_map(
        per_device,
        mesh=mesh,
        in_specs=placed,
        out_specs=(P("grp", "tp"), P("grp", "tp")),
        check_vma=False,
    )
```

```python
import jax
import jax.numpy as jnp
from jax import lax
from jax.experimental import pallas as pl
from jax.experimental.pallas import tpu as pltpu
from jax.sharding import PartitionSpec as P

QH = 64
KVH = 8
HD = 128
HEADS = QH // KVH

BF = jnp.bfloat16
F32 = jnp.float32
SMEM = pl.BlockSpec(memory_space=pltpu.SMEM)
VMEM = pl.BlockSpec(memory_space=pltpu.VMEM)
ANY = pl.BlockSpec(memory_space=pl.ANY)


SMALL = pltpu.CompilerParams(vmem_limit_bytes=8 << 20)


def near(array):
    return pltpu.with_memory_space_constraint(array, pltpu.VMEM)


def empty_slot_of(slot_ref):
    found = jnp.int32(0)
    for s in range(slot_ref.shape[0]):
        found = jnp.where(slot_ref[s] < 0, jnp.int32(s), found)
    return found


def look_up(moves_ref, own, key, fields):
    hit_any = jnp.int32(0)
    values = [jnp.int32(0) for _ in fields]
    for i in range(moves_ref.shape[0]):
        hit = moves_ref[i, key] == own
        hit_any = jnp.where(hit, jnp.int32(1), hit_any)
        values = [jnp.where(hit, moves_ref[i, f], v) for f, v in zip(fields, values)]
    return hit_any, values


def fact(facts_ref, k):
    lane = lax.broadcasted_iota(jnp.int32, facts_ref.shape, 1)
    return jnp.sum(jnp.where(lane == k, facts_ref[...], 0.0)).astype(jnp.int32)


def offer_kernel(
    own_ref,
    len_ref,
    slot_ref,
    moves_ref,
    query_ref,
    fresh_ref,
    prompt_ref,
    suffix_ref,
    out_ref,
    near_prompt_ref,
    near_suffix_ref,
    facts_ref,
    sems,
):
    copies = (
        pltpu.make_async_copy(prompt_ref, near_prompt_ref, sems.at[0]),
        pltpu.make_async_copy(suffix_ref, near_suffix_ref, sems.at[1]),
    )
    for copy in copies:
        copy.start()
    own = own_ref[0]
    slots = query_ref.shape[0]
    empty = empty_slot_of(slot_ref)
    is_source, (out_slot, destination) = look_up(moves_ref, own, 0, (1, 2))
    is_target, (in_source,) = look_up(moves_ref, own, 2, (0,))
    facts = (
        destination,
        2 * len_ref[own * slots + out_slot],
        out_slot,
        jnp.maximum(slot_ref[out_slot], 0),
        in_source,
        jnp.where(is_target == 1, slots + empty, -1),
    )
    lane = lax.broadcasted_iota(jnp.int32, facts_ref.shape, 1)
    held = jnp.zeros(facts_ref.shape, jnp.int32)
    for k, value in enumerate(facts):
        held = jnp.where(lane == k, value, held)
    facts_ref[...] = held.astype(F32)
    mine = lax.broadcasted_iota(jnp.int32, (slots, HD), 0) == empty
    rows = []
    for h in range(HEADS):
        part = query_ref[:, h * HD : (h + 1) * HD].astype(F32)
        rows.append(jnp.sum(jnp.where(mine, part, 0.0), axis=0, keepdims=True))
    pair = jnp.zeros((2, HD), F32)
    for s in range(slots):
        pair = jnp.where(empty == s, fresh_ref[s].astype(F32), pair)
    rows += [pair, jnp.zeros((6, HD), F32)]
    block = jnp.concatenate(rows, axis=0).astype(BF)
    out_ref[...] = jnp.broadcast_to(block[None], out_ref.shape)
    for copy in copies:
        copy.wait()


def attend(queries, cached, pairs):
    scale = HD ** (-0.5)
    narrow = queries.astype(BF)
    row = lax.broadcasted_iota(jnp.int32, (queries.shape[0], 1), 0)
    scores = []
    for rows, width in cached:
        score = (
            lax.dot_general(
                narrow, rows, (((1,), (1,)), ((), ())), preferred_element_type=F32
            )
            * scale
        )
        column = lax.broadcasted_iota(jnp.int32, score.shape, 1)
        counts = column % 2 == 0
        if width is not None:
            counts = counts & (column < width)
        scores.append(jnp.where(counts, score, -1e30))
    singles = []
    for pair, since in pairs:
        score = jnp.sum(queries * pair[0:1], axis=1, keepdims=True) * scale
        singles.append(jnp.where(row >= since, score, -1e30) if since else score)
    highest = singles[0]
    for score in singles[1:]:
        highest = jnp.maximum(highest, score)
    for score in scores:
        highest = jnp.maximum(highest, jnp.max(score, axis=1, keepdims=True))
    spreads = [jnp.exp(score - highest) for score in scores]
    single_spreads = [jnp.exp(score - highest) for score in singles]
    total = sum(single_spreads)
    for spread in spreads:
        total = total + jnp.sum(spread, axis=1, keepdims=True)
    share = 1.0 / total
    mixed = jnp.zeros(queries.shape, F32)
    for (rows, _), spread in zip(cached, spreads):
        weights = pltpu.roll(spread * share, 1, 1).astype(BF)
        mixed += lax.dot(weights, rows, preferred_element_type=F32)
    for (pair, _), spread in zip(pairs, single_spreads):
        mixed += (spread * share).astype(BF).astype(F32) * pair[1:2]
    return mixed.astype(BF)


def stay_kernel(
    own_ref,
    len_ref,
    slot_ref,
    moves_ref,
    query_first_ref,
    query_second_ref,
    fresh_first_ref,
    fresh_second_ref,
    prompt_ref,
    suffix_ref,
    rows_ref,
    pair_ref,
    queries_ref,
):
    own = own_ref[0]
    slots = query_first_ref.shape[0]
    is_source, (out_slot,) = look_up(moves_ref, own, 0, (1,))
    for h in range(HEADS):
        queries_ref[:, h, :] = query_first_ref[:, h * HD : (h + 1) * HD].astype(F32)
        queries_ref[:, HEADS + h, :] = query_second_ref[:, h * HD : (h + 1) * HD].astype(F32)
    pair_ref[...] = fresh_first_ref[out_slot].astype(F32)
    for s in range(slots):
        prompt_id = slot_ref[s]
        live = prompt_id >= 0
        stays = live & jnp.logical_not((is_source == 1) & (out_slot == s))
        mixed = attend(
            queries_ref[s],
            (
                (prompt_ref[jnp.maximum(prompt_id, 0)], None),
                (suffix_ref[s], 2 * len_ref[own * slots + s]),
            ),
            ((fresh_first_ref[s].astype(F32), 0), (fresh_second_ref[s].astype(F32), HEADS)),
        ).astype(F32)
        rows_ref[:, s, :] = jnp.where(live, mixed[:HEADS], 0.0)
        rows_ref[:, slots + s, :] = jnp.where(stays, mixed[HEADS:], 0.0)


def leave_kernel(facts_ref, offers_ref, prompt_ref, suffix_ref, pair_ref, moved_ref):
    offer = offers_ref[fact(facts_ref, 0)].astype(F32)
    mixed = attend(
        offer[:HEADS],
        (
            (prompt_ref[fact(facts_ref, 3)], None),
            (suffix_ref[fact(facts_ref, 2)], fact(facts_ref, 1)),
        ),
        ((pair_ref[...], 0), (offer[HEADS : HEADS + 2], 0)),
    )
    moved_ref[...] = jnp.broadcast_to(mixed[None], moved_ref.shape)


def merge_kernel(facts_ref, rows_ref, arrived_ref, out_ref):
    arrived = arrived_ref[fact(facts_ref, 4)].astype(F32)
    into = lax.broadcasted_iota(jnp.int32, rows_ref.shape[1:], 0) == fact(facts_ref, 5)
    for h in range(HEADS):
        row = jnp.where(into, arrived[h : h + 1], rows_ref[h])
        out_ref[:, h * HD : (h + 1) * HD] = row.astype(BF)


def sum_kernel(parts_ref, first_ref, second_ref):
    total = jnp.sum(parts_ref[...], axis=0)
    slots = first_ref.shape[0]
    first_ref[...] = total[:slots].astype(BF)
    second_ref[...] = total[slots:].astype(BF)


def per_device(
    suffix_cache,
    prompt_cache,
    query_first,
    fresh_first,
    query_second,
    fresh_second,
    out_weight,
    suffix_len,
    prompt_slot,
    moves,
):
    slots, cap = suffix_cache.shape[:2]
    prompts, prompt_len = prompt_cache.shape[:2]
    groups = lax.axis_size("grp")
    shares = lax.axis_size("tp")
    features = out_weight.shape[1]
    own = lax.axis_index("grp").astype(jnp.int32).reshape(1)
    suffix_rows = suffix_cache.reshape(slots, 2 * cap, HD)
    prompt_rows = prompt_cache.reshape(prompts, 2 * prompt_len, HD)
    offer, near_prompt, near_suffix, facts = pl.pallas_call(
        offer_kernel,
        out_shape=(
            pltpu.VMEM((groups, 2 * HEADS, HD), BF),
            pltpu.VMEM(prompt_rows.shape, BF),
            pltpu.VMEM(suffix_rows.shape, BF),
            pltpu.VMEM((1, HD), F32),
        ),
        in_specs=[SMEM] * 4 + [VMEM] * 2 + [ANY] * 2,
        out_specs=(VMEM,) * 4,
        scratch_shapes=[pltpu.SemaphoreType.DMA((2,))],
        name="offer",
    )(
        own,
        suffix_len,
        prompt_slot,
        moves,
        query_second,
        fresh_second,
        prompt_rows,
        suffix_rows,
    )
    offers = lax.all_to_all(offer, "grp", 0, 0, tiled=True)
    rows, pair = pl.pallas_call(
        stay_kernel,
        out_shape=(pltpu.VMEM((HEADS, 2 * slots, HD), F32), pltpu.VMEM((2, HD), F32)),
        in_specs=[SMEM] * 4 + [VMEM] * 6,
        out_specs=(VMEM, VMEM),
        scratch_shapes=[pltpu.VMEM((slots, 2 * HEADS, HD), F32)],
        name="stay",
    )(
        own,
        suffix_len,
        prompt_slot,
        moves,
        query_first,
        query_second,
        fresh_first,
        fresh_second,
        near(near_prompt),
        near(near_suffix),
    )
    moved = pl.pallas_call(
        leave_kernel,
        out_shape=pltpu.VMEM((groups, HEADS, HD), BF),
        in_specs=[VMEM] * 5,
        out_specs=VMEM,
        compiler_params=SMALL,
        cost_estimate=pl.CostEstimate(flops=10**11, transcendentals=0, bytes_accessed=1 << 20),
        name="leave",
    )(near(facts), near(offers), near(near_prompt), near(near_suffix), near(pair))
    arrived = lax.all_to_all(moved, "grp", 0, 0, tiled=True)
    merged = pl.pallas_call(
        merge_kernel,
        out_shape=pltpu.VMEM((2 * slots, HEADS * HD), BF),
        in_specs=[VMEM] * 3,
        out_specs=VMEM,
        compiler_params=SMALL,
        name="merge",
    )(near(facts), near(rows), near(arrived))
    parts = jnp.dot(merged, out_weight, preferred_element_type=F32)
    parts = parts.reshape(2 * slots, shares, features // shares).swapaxes(0, 1)
    parts = lax.all_to_all(parts, "tp", 0, 0, tiled=True)
    out = jax.ShapeDtypeStruct((slots, features // shares), BF)
    return pl.pallas_call(
        sum_kernel,
        out_shape=(out, out),
        in_specs=[VMEM],
        out_specs=(VMEM, VMEM),
        compiler_params=SMALL,
        name="sum",
    )(near(parts))


def solution(mesh):
    placed = (
        P("grp", None, None, "tp"),
        P("grp", None, None, "tp"),
        P("grp", "tp"),
        P("grp", None, "tp"),
        P("grp", "tp"),
        P("grp", None, "tp"),
        P("tp", None),
        P(),
        P("grp"),
        P(),
    )
    return jax.shard_map(
        per_device,
        mesh=mesh,
        in_specs=placed,
        out_specs=(P("grp", "tp"), P("grp", "tp")),
        check_vma=False,
    )
```

```python
import jax
import jax.numpy as jnp
from jax import lax
from jax.experimental import pallas as pl
from jax.experimental.pallas import tpu as pltpu
from jax.sharding import PartitionSpec as P

QH = 64
KVH = 8
HD = 128
HEADS = QH // KVH

BF = jnp.bfloat16
F32 = jnp.float32
SMEM = pl.BlockSpec(memory_space=pltpu.SMEM)
VMEM = pl.BlockSpec(memory_space=pltpu.VMEM)
ANY = pl.BlockSpec(memory_space=pl.ANY)


SMALL = pltpu.CompilerParams(vmem_limit_bytes=8 << 20)


def near(array):
    return pltpu.with_memory_space_constraint(array, pltpu.VMEM)


def empty_slot_of(slot_ref):
    found = jnp.int32(0)
    for s in range(slot_ref.shape[0]):
        found = jnp.where(slot_ref[s] < 0, jnp.int32(s), found)
    return found


def look_up(moves_ref, own, key, fields):
    hit_any = jnp.int32(0)
    values = [jnp.int32(0) for _ in fields]
    for i in range(moves_ref.shape[0]):
        hit = moves_ref[i, key] == own
        hit_any = jnp.where(hit, jnp.int32(1), hit_any)
        values = [jnp.where(hit, moves_ref[i, f], v) for f, v in zip(fields, values)]
    return hit_any, values


def fact(facts_ref, k):
    lane = lax.broadcasted_iota(jnp.int32, facts_ref.shape, 1)
    return jnp.sum(jnp.where(lane == k, facts_ref[...], 0.0)).astype(jnp.int32)


def offer_kernel(slot_ref, query_ref, fresh_ref, out_ref):
    empty = empty_slot_of(slot_ref)
    slots = query_ref.shape[0]
    mine = lax.broadcasted_iota(jnp.int32, (slots, HD), 0) == empty
    rows = []
    for h in range(HEADS):
        part = query_ref[:, h * HD : (h + 1) * HD].astype(F32)
        rows.append(jnp.sum(jnp.where(mine, part, 0.0), axis=0, keepdims=True))
    pair = jnp.zeros((2, HD), F32)
    for s in range(slots):
        pair = jnp.where(empty == s, fresh_ref[s].astype(F32), pair)
    rows += [pair, jnp.zeros((6, HD), F32)]
    block = jnp.concatenate(rows, axis=0).astype(BF)
    out_ref[...] = jnp.broadcast_to(block[None], out_ref.shape)


def attend(queries, cached, pairs):
    scale = HD ** (-0.5)
    narrow = queries.astype(BF)
    row = lax.broadcasted_iota(jnp.int32, (queries.shape[0], 1), 0)
    scores = []
    for rows, width in cached:
        score = (
            lax.dot_general(
                narrow, rows, (((1,), (1,)), ((), ())), preferred_element_type=F32
            )
            * scale
        )
        column = lax.broadcasted_iota(jnp.int32, score.shape, 1)
        counts = column % 2 == 0
        if width is not None:
            counts = counts & (column < width)
        scores.append(jnp.where(counts, score, -1e30))
    singles = []
    for pair, since in pairs:
        score = jnp.sum(queries * pair[0:1], axis=1, keepdims=True) * scale
        singles.append(jnp.where(row >= since, score, -1e30) if since else score)
    highest = singles[0]
    for score in singles[1:]:
        highest = jnp.maximum(highest, score)
    for score in scores:
        highest = jnp.maximum(highest, jnp.max(score, axis=1, keepdims=True))
    spreads = [jnp.exp(score - highest) for score in scores]
    single_spreads = [jnp.exp(score - highest) for score in singles]
    total = sum(single_spreads)
    for spread in spreads:
        total = total + jnp.sum(spread, axis=1, keepdims=True)
    share = 1.0 / total
    mixed = jnp.zeros(queries.shape, F32)
    for (rows, _), spread in zip(cached, spreads):
        weights = pltpu.roll(spread * share, 1, 1).astype(BF)
        mixed += lax.dot(weights, rows, preferred_element_type=F32)
    for (pair, _), spread in zip(pairs, single_spreads):
        mixed += (spread * share).astype(BF).astype(F32) * pair[1:2]
    return mixed.astype(BF)


def stay_kernel(
    own_ref,
    len_ref,
    slot_ref,
    moves_ref,
    query_first_ref,
    query_second_ref,
    fresh_first_ref,
    fresh_second_ref,
    far_prompt_ref,
    far_suffix_ref,
    rows_ref,
    pair_ref,
    prompt_ref,
    suffix_ref,
    facts_ref,
    queries_ref,
    sems,
):
    own = own_ref[0]
    slots = query_first_ref.shape[0]
    prompt_copy = pltpu.make_async_copy(far_prompt_ref, prompt_ref, sems.at[slots])
    suffix_copies = [
        pltpu.make_async_copy(far_suffix_ref.at[s], suffix_ref.at[s], sems.at[s])
        for s in range(slots)
    ]
    prompt_copy.start()
    for copy in suffix_copies:
        copy.start()
    is_source, (out_slot, destination) = look_up(moves_ref, own, 0, (1, 2))
    is_target, (in_source,) = look_up(moves_ref, own, 2, (0,))
    facts = (
        destination,
        2 * len_ref[own * slots + out_slot],
        out_slot,
        jnp.maximum(slot_ref[out_slot], 0),
        in_source,
        jnp.where(is_target == 1, slots + empty_slot_of(slot_ref), -1),
    )
    lane = lax.broadcasted_iota(jnp.int32, facts_ref.shape, 1)
    held = jnp.zeros(facts_ref.shape, jnp.int32)
    for k, value in enumerate(facts):
        held = jnp.where(lane == k, value, held)
    facts_ref[...] = held.astype(F32)
    for h in range(HEADS):
        queries_ref[:, h, :] = query_first_ref[:, h * HD : (h + 1) * HD].astype(F32)
        queries_ref[:, HEADS + h, :] = query_second_ref[:, h * HD : (h + 1) * HD].astype(F32)
    pair_ref[...] = fresh_first_ref[out_slot].astype(F32)
    prompt_copy.wait()
    for copy in suffix_copies:
        copy.wait()
    for s in range(slots):
        prompt_id = slot_ref[s]
        live = prompt_id >= 0
        stays = live & jnp.logical_not((is_source == 1) & (out_slot == s))
        mixed = attend(
            queries_ref[s],
            (
                (prompt_ref[jnp.maximum(prompt_id, 0)], None),
                (suffix_ref[s], 2 * len_ref[own * slots + s]),
            ),
            ((fresh_first_ref[s].astype(F32), 0), (fresh_second_ref[s].astype(F32), HEADS)),
        ).astype(F32)
        rows_ref[:, s, :] = jnp.where(live, mixed[:HEADS], 0.0)
        rows_ref[:, slots + s, :] = jnp.where(stays, mixed[HEADS:], 0.0)


def leave_kernel(facts_ref, offers_ref, prompt_ref, suffix_ref, pair_ref, moved_ref):
    offer = offers_ref[fact(facts_ref, 0)].astype(F32)
    mixed = attend(
        offer[:HEADS],
        (
            (prompt_ref[fact(facts_ref, 3)], None),
            (suffix_ref[fact(facts_ref, 2)], fact(facts_ref, 1)),
        ),
        ((pair_ref[...], 0), (offer[HEADS : HEADS + 2], 0)),
    )
    moved_ref[...] = jnp.broadcast_to(mixed[None], moved_ref.shape)


def merge_kernel(facts_ref, rows_ref, arrived_ref, out_ref):
    arrived = arrived_ref[fact(facts_ref, 4)].astype(F32)
    into = lax.broadcasted_iota(jnp.int32, rows_ref.shape[1:], 0) == fact(facts_ref, 5)
    for h in range(HEADS):
        row = jnp.where(into, arrived[h : h + 1], rows_ref[h])
        out_ref[:, h * HD : (h + 1) * HD] = row.astype(BF)


def sum_kernel(parts_ref, first_ref, second_ref):
    total = jnp.sum(parts_ref[...], axis=0)
    slots = first_ref.shape[0]
    first_ref[...] = total[:slots].astype(BF)
    second_ref[...] = total[slots:].astype(BF)


def per_device(
    suffix_cache,
    prompt_cache,
    query_first,
    fresh_first,
    query_second,
    fresh_second,
    out_weight,
    suffix_len,
    prompt_slot,
    moves,
):
    slots, cap = suffix_cache.shape[:2]
    prompts, prompt_len = prompt_cache.shape[:2]
    groups = lax.axis_size("grp")
    shares = lax.axis_size("tp")
    features = out_weight.shape[1]
    own = lax.axis_index("grp").astype(jnp.int32).reshape(1)
    suffix_rows = suffix_cache.reshape(slots, 2 * cap, HD)
    prompt_rows = prompt_cache.reshape(prompts, 2 * prompt_len, HD)
    offer = pl.pallas_call(
        offer_kernel,
        out_shape=pltpu.VMEM((groups, 2 * HEADS, HD), BF),
        in_specs=[SMEM, VMEM, VMEM],
        out_specs=VMEM,
        name="offer",
    )(prompt_slot, query_second, fresh_second)
    offers = lax.all_to_all(offer, "grp", 0, 0, tiled=True)
    rows, pair, near_prompt, near_suffix, facts = pl.pallas_call(
        stay_kernel,
        out_shape=(
            pltpu.VMEM((HEADS, 2 * slots, HD), F32),
            pltpu.VMEM((2, HD), F32),
            pltpu.VMEM(prompt_rows.shape, BF),
            pltpu.VMEM(suffix_rows.shape, BF),
            pltpu.VMEM((1, HD), F32),
        ),
        in_specs=[SMEM] * 4 + [VMEM] * 4 + [ANY] * 2,
        out_specs=(VMEM,) * 5,
        scratch_shapes=[
            pltpu.VMEM((slots, 2 * HEADS, HD), F32),
            pltpu.SemaphoreType.DMA((slots + 1,)),
        ],
        name="stay",
    )(
        own,
        suffix_len,
        prompt_slot,
        moves,
        query_first,
        query_second,
        fresh_first,
        fresh_second,
        prompt_rows,
        suffix_rows,
    )
    moved = pl.pallas_call(
        leave_kernel,
        out_shape=pltpu.VMEM((groups, HEADS, HD), BF),
        in_specs=[VMEM] * 5,
        out_specs=VMEM,
        compiler_params=SMALL,
        cost_estimate=pl.CostEstimate(flops=10**11, transcendentals=0, bytes_accessed=1 << 20),
        name="leave",
    )(near(facts), near(offers), near(near_prompt), near(near_suffix), near(pair))
    arrived = lax.all_to_all(moved, "grp", 0, 0, tiled=True)
    merged = pl.pallas_call(
        merge_kernel,
        out_shape=pltpu.VMEM((2 * slots, HEADS * HD), BF),
        in_specs=[VMEM] * 3,
        out_specs=VMEM,
        compiler_params=SMALL,
        name="merge",
    )(near(facts), near(rows), near(arrived))
    parts = jnp.dot(merged, out_weight, preferred_element_type=F32)
    parts = parts.reshape(2 * slots, shares, features // shares).swapaxes(0, 1)
    parts = lax.all_to_all(parts, "tp", 0, 0, tiled=True)
    out = jax.ShapeDtypeStruct((slots, features // shares), BF)
    return pl.pallas_call(
        sum_kernel,
        out_shape=(out, out),
        in_specs=[VMEM],
        out_specs=(VMEM, VMEM),
        compiler_params=SMALL,
        name="sum",
    )(near(parts))


def solution(mesh):
    placed = (
        P("grp", None, None, "tp"),
        P("grp", None, None, "tp"),
        P("grp", "tp"),
        P("grp", None, "tp"),
        P("grp", "tp"),
        P("grp", None, "tp"),
        P("tp", None),
        P(),
        P("grp"),
        P(),
    )
    return jax.shard_map(
        per_device,
        mesh=mesh,
        in_specs=placed,
        out_specs=(P("grp", "tp"), P("grp", "tp")),
        check_vma=False,
    )
```

```python
import functools

import jax
import jax.numpy as jnp
from jax import lax
from jax.experimental import pallas as pl
from jax.experimental.pallas import tpu as pltpu
from jax.sharding import PartitionSpec as P

QH = 64
KVH = 8
HD = 128
HEADS = QH // KVH

BF = jnp.bfloat16
F32 = jnp.float32
SMEM = pl.BlockSpec(memory_space=pltpu.SMEM)
VMEM = pl.BlockSpec(memory_space=pltpu.VMEM)
ANY = pl.BlockSpec(memory_space=pl.ANY)


SMALL = pltpu.CompilerParams(vmem_limit_bytes=8 << 20)


def near(array):
    return pltpu.with_memory_space_constraint(array, pltpu.VMEM)


def empty_slot_of(slot_ref):
    found = jnp.int32(0)
    for s in range(slot_ref.shape[0]):
        found = jnp.where(slot_ref[s] < 0, jnp.int32(s), found)
    return found


def look_up(moves_ref, own, key, fields):
    hit_any = jnp.int32(0)
    values = [jnp.int32(0) for _ in fields]
    for i in range(moves_ref.shape[0]):
        hit = moves_ref[i, key] == own
        hit_any = jnp.where(hit, jnp.int32(1), hit_any)
        values = [jnp.where(hit, moves_ref[i, f], v) for f, v in zip(fields, values)]
    return hit_any, values


def fact(facts_ref, k):
    lane = lax.broadcasted_iota(jnp.int32, facts_ref.shape, 1)
    return jnp.sum(jnp.where(lane == k, facts_ref[...], 0.0)).astype(jnp.int32)


def offer_kernel(slot_ref, query_ref, fresh_ref, out_ref):
    empty = empty_slot_of(slot_ref)
    slots = query_ref.shape[0]
    mine = lax.broadcasted_iota(jnp.int32, (slots, HD), 0) == empty
    rows = []
    for h in range(HEADS):
        part = query_ref[:, h * HD : (h + 1) * HD].astype(F32)
        rows.append(jnp.sum(jnp.where(mine, part, 0.0), axis=0, keepdims=True))
    pair = jnp.zeros((2, HD), F32)
    for s in range(slots):
        pair = jnp.where(empty == s, fresh_ref[s].astype(F32), pair)
    rows += [pair, jnp.zeros((6, HD), F32)]
    block = jnp.concatenate(rows, axis=0).astype(BF)
    out_ref[...] = jnp.broadcast_to(block[None], out_ref.shape)


def attend(samples, width_of_rows):
    scale = HD ** (-0.5)
    shape = (samples[0][0].shape[0], width_of_rows)
    column = lax.broadcasted_iota(jnp.int32, shape, 1)
    on_key = column % 2 == 0
    limit = jnp.where(on_key, -1, column)
    row = lax.broadcasted_iota(jnp.int32, (shape[0], 1), 0)
    contract_last = (((1,), (1,)), ((), ()))
    raw = []
    for queries, prompt, suffix, _, _, waits in samples:
        for wait in waits:
            wait()
        narrow = queries.astype(BF)
        raw.append(
            tuple(
                lax.dot_general(narrow, rows, contract_last, preferred_element_type=F32)
                for rows in (prompt(), suffix())
            )
        )
    held = []
    for (queries, _, _, width, pairs, _), (on_prompt, on_suffix) in zip(samples, raw):
        scores = jnp.where(on_key, on_prompt, pltpu.roll(on_suffix, 1, 1)) * scale
        scores = jnp.where(limit < width, scores, -1e30)
        singles = []
        for pair, since in pairs:
            score = jnp.sum(queries * pair[0:1], axis=1, keepdims=True) * scale
            singles.append(jnp.where(row >= since, score, -1e30) if since else score)
        highest = jnp.max(scores, axis=1, keepdims=True)
        for score in singles:
            highest = jnp.maximum(highest, score)
        spread = jnp.exp(scores - highest)
        single_spreads = [jnp.exp(score - highest) for score in singles]
        share = 1.0 / (jnp.sum(spread, axis=1, keepdims=True) + sum(single_spreads))
        weights = spread * share
        held.append(
            (
                jnp.where(on_key, 0.0, pltpu.roll(weights, 1, 1)).astype(BF),
                jnp.where(on_key, 0.0, weights).astype(BF),
                [(spread * share).astype(BF).astype(F32) for spread in single_spreads],
            )
        )
    results = []
    for (_, prompt, suffix, _, pairs, _), (prompt_weights, suffix_weights, single_weights) in zip(
        samples, held
    ):
        mixed = lax.dot(prompt_weights, prompt(), preferred_element_type=F32)
        mixed += lax.dot(suffix_weights, suffix(), preferred_element_type=F32)
        for (pair, _), weight in zip(pairs, single_weights):
            mixed += weight * pair[1:2]
        results.append(mixed.astype(BF))
    return results


def stay_kernel(*refs):
    far_prompt_ref, far_suffix_ref, *far_refs = refs[:9]
    rows_ref, pair_ref, prompt_ref, suffix_ref, facts_ref = refs[9:14]
    queries_ref, *near_refs, sems = refs[14:]
    slots = suffix_ref.shape[0]
    prompt_copy = pltpu.make_async_copy(far_prompt_ref, prompt_ref, sems.at[slots])
    suffix_copies = [
        pltpu.make_async_copy(far_suffix_ref.at[s], suffix_ref.at[s], sems.at[s])
        for s in range(slots)
    ]
    small_copies = [
        pltpu.make_async_copy(far, close, sems.at[slots + 1 + k])
        for k, (far, close) in enumerate(zip(far_refs, near_refs))
    ]
    for copy in (*small_copies, prompt_copy, *suffix_copies):
        copy.start()
    own = lax.axis_index("grp")
    for copy in small_copies:
        copy.wait()
    len_ref, slot_ref, moves_ref = near_refs[:3]
    query_first_ref, query_second_ref, fresh_first_ref, fresh_second_ref = near_refs[3:]
    is_source, (out_slot, destination) = look_up(moves_ref, own, 0, (1, 2))
    is_target, (in_source,) = look_up(moves_ref, own, 2, (0,))
    facts = (
        destination,
        2 * len_ref[own * slots + out_slot],
        out_slot,
        jnp.maximum(slot_ref[out_slot], 0),
        in_source,
        jnp.where(is_target == 1, slots + empty_slot_of(slot_ref), -1),
    )
    lane = lax.broadcasted_iota(jnp.int32, facts_ref.shape, 1)
    held = jnp.zeros(facts_ref.shape, jnp.int32)
    for k, value in enumerate(facts):
        held = jnp.where(lane == k, value, held)
    facts_ref[...] = held.astype(F32)
    for h in range(HEADS):
        queries_ref[:, h, :] = query_first_ref[:, h * HD : (h + 1) * HD].astype(F32)
        queries_ref[:, HEADS + h, :] = query_second_ref[:, h * HD : (h + 1) * HD].astype(F32)
    pair_ref[...] = fresh_first_ref[out_slot].astype(F32)
    mixed = attend(
        [
            (
                queries_ref[s],
                functools.partial(prompt_ref.__getitem__, jnp.maximum(slot_ref[s], 0)),
                functools.partial(suffix_ref.__getitem__, s),
                2 * len_ref[own * slots + s],
                ((fresh_first_ref[s].astype(F32), 0), (fresh_second_ref[s].astype(F32), HEADS)),
                [suffix_copies[s].wait] if s else [prompt_copy.wait, suffix_copies[0].wait],
            )
            for s in range(slots)
        ],
        suffix_ref.shape[1],
    )
    for s in range(slots):
        live = slot_ref[s] >= 0
        stays = live & jnp.logical_not((is_source == 1) & (out_slot == s))
        row = mixed[s].astype(F32)
        rows_ref[:, s, :] = jnp.where(live, row[:HEADS], 0.0)
        rows_ref[:, slots + s, :] = jnp.where(stays, row[HEADS:], 0.0)


def leave_kernel(facts_ref, offers_ref, prompt_ref, suffix_ref, pair_ref, moved_ref):
    offer = offers_ref[fact(facts_ref, 0)].astype(F32)
    (mixed,) = attend(
        [
            (
                offer[:HEADS],
                functools.partial(prompt_ref.__getitem__, fact(facts_ref, 3)),
                functools.partial(suffix_ref.__getitem__, fact(facts_ref, 2)),
                fact(facts_ref, 1),
                ((pair_ref[...], 0), (offer[HEADS : HEADS + 2], 0)),
                [],
            )
        ],
        suffix_ref.shape[1],
    )
    moved_ref[...] = jnp.broadcast_to(mixed[None], moved_ref.shape)


def merge_kernel(facts_ref, rows_ref, arrived_ref, out_ref):
    arrived = arrived_ref[fact(facts_ref, 4)].astype(F32)
    into = lax.broadcasted_iota(jnp.int32, rows_ref.shape[1:], 0) == fact(facts_ref, 5)
    for h in range(HEADS):
        row = jnp.where(into, arrived[h : h + 1], rows_ref[h])
        out_ref[:, h * HD : (h + 1) * HD] = row.astype(BF)


def sum_kernel(parts_ref, first_ref, second_ref):
    total = jnp.sum(parts_ref[...], axis=0)
    slots = first_ref.shape[0]
    first_ref[...] = total[:slots].astype(BF)
    second_ref[...] = total[slots:].astype(BF)


def per_device(
    suffix_cache,
    prompt_cache,
    query_first,
    fresh_first,
    query_second,
    fresh_second,
    out_weight,
    suffix_len,
    prompt_slot,
    moves,
):
    slots, cap = suffix_cache.shape[:2]
    prompts, prompt_len = prompt_cache.shape[:2]
    groups = lax.axis_size("grp")
    shares = lax.axis_size("tp")
    features = out_weight.shape[1]
    suffix_rows = suffix_cache.reshape(slots, 2 * cap, HD)
    prompt_rows = prompt_cache.reshape(prompts, 2 * prompt_len, HD)
    offer = pl.pallas_call(
        offer_kernel,
        out_shape=pltpu.VMEM((groups, 2 * HEADS, HD), BF),
        in_specs=[SMEM, VMEM, VMEM],
        out_specs=VMEM,
        name="offer",
    )(prompt_slot, query_second, fresh_second)
    offers = lax.all_to_all(offer, "grp", 0, 0, tiled=True)
    tables = (suffix_len, prompt_slot, moves)
    vectors = (query_first, query_second, fresh_first, fresh_second)
    rows, pair, near_prompt, near_suffix, facts = pl.pallas_call(
        stay_kernel,
        out_shape=(
            pltpu.VMEM((HEADS, 2 * slots, HD), F32),
            pltpu.VMEM((2, HD), F32),
            pltpu.VMEM(prompt_rows.shape, BF),
            pltpu.VMEM(suffix_rows.shape, BF),
            pltpu.VMEM((1, HD), F32),
        ),
        in_specs=[ANY] * 9,
        out_specs=(VMEM,) * 5,
        scratch_shapes=[
            pltpu.VMEM((slots, 2 * HEADS, HD), F32),
            *(pltpu.SMEM(table.shape, jnp.int32) for table in tables),
            *(pltpu.VMEM(array.shape, BF) for array in vectors),
            pltpu.SemaphoreType.DMA((slots + 1 + len(tables) + len(vectors),)),
        ],
        name="stay",
    )(prompt_rows, suffix_rows, *tables, *vectors)
    moved = pl.pallas_call(
        leave_kernel,
        out_shape=pltpu.VMEM((groups, HEADS, HD), BF),
        in_specs=[VMEM] * 5,
        out_specs=VMEM,
        compiler_params=SMALL,
        cost_estimate=pl.CostEstimate(flops=10**11, transcendentals=0, bytes_accessed=1 << 20),
        name="leave",
    )(near(facts), near(offers), near(near_prompt), near(near_suffix), near(pair))
    arrived = lax.all_to_all(moved, "grp", 0, 0, tiled=True)
    merged = pl.pallas_call(
        merge_kernel,
        out_shape=pltpu.VMEM((2 * slots, HEADS * HD), BF),
        in_specs=[VMEM] * 3,
        out_specs=VMEM,
        compiler_params=SMALL,
        name="merge",
    )(near(facts), near(rows), near(arrived))
    parts = jnp.dot(merged, out_weight, preferred_element_type=F32)
    parts = parts.reshape(2 * slots, shares, features // shares).swapaxes(0, 1)
    parts = lax.all_to_all(parts, "tp", 0, 0, tiled=True)
    out = jax.ShapeDtypeStruct((slots, features // shares), BF)
    return pl.pallas_call(
        sum_kernel,
        out_shape=(out, out),
        in_specs=[VMEM],
        out_specs=(VMEM, VMEM),
        compiler_params=SMALL,
        name="sum",
    )(near(parts))


def solution(mesh):
    placed = (
        P("grp", None, None, "tp"),
        P("grp", None, None, "tp"),
        P("grp", "tp"),
        P("grp", None, "tp"),
        P("grp", "tp"),
        P("grp", None, "tp"),
        P("tp", None),
        P(),
        P("grp"),
        P(),
    )
    return jax.shard_map(
        per_device,
        mesh=mesh,
        in_specs=placed,
        out_specs=(P("grp", "tp"), P("grp", "tp")),
        check_vma=False,
    )
```

```python
import functools

import jax
import jax.numpy as jnp
from jax import lax
from jax.experimental import pallas as pl
from jax.experimental.pallas import tpu as pltpu
from jax.sharding import PartitionSpec as P

QH = 64
KVH = 8
HD = 128
HEADS = QH // KVH

BF = jnp.bfloat16
F32 = jnp.float32
SMEM = pl.BlockSpec(memory_space=pltpu.SMEM)
VMEM = pl.BlockSpec(memory_space=pltpu.VMEM)
ANY = pl.BlockSpec(memory_space=pl.ANY)


SMALL = pltpu.CompilerParams(vmem_limit_bytes=8 << 20)


def near(array):
    return pltpu.with_memory_space_constraint(array, pltpu.VMEM)


def empty_slot_of(slot_ref):
    found = jnp.int32(0)
    for s in range(slot_ref.shape[0]):
        found = jnp.where(slot_ref[s] < 0, jnp.int32(s), found)
    return found


def look_up(moves_ref, own, key, fields):
    hit_any = jnp.int32(0)
    values = [jnp.int32(0) for _ in fields]
    for i in range(moves_ref.shape[0]):
        hit = moves_ref[i, key] == own
        hit_any = jnp.where(hit, jnp.int32(1), hit_any)
        values = [jnp.where(hit, moves_ref[i, f], v) for f, v in zip(fields, values)]
    return hit_any, values


def fact(facts_ref, k):
    lane = lax.broadcasted_iota(jnp.int32, facts_ref.shape, 1)
    return jnp.sum(jnp.where(lane == k, facts_ref[...], 0.0)).astype(jnp.int32)


def offer_kernel(slot_ref, query_ref, fresh_ref, out_ref):
    empty = empty_slot_of(slot_ref)
    slots = query_ref.shape[0]
    half = query_ref.shape[1] // 2
    mine = lax.broadcasted_iota(jnp.int32, (slots, half), 0) == empty
    pair = jnp.zeros((2, HD), F32)
    for s in range(slots):
        pair = jnp.where(empty == s, fresh_ref[s].astype(F32), pair)
    rows = []
    for r in range(2):
        part = query_ref[:, r * half : (r + 1) * half].astype(F32)
        heads = jnp.sum(jnp.where(mine, part, 0.0), axis=0, keepdims=True)
        rows.append(jnp.concatenate([heads, pair[r : r + 1]], axis=1))
    block = jnp.concatenate(rows, axis=0).astype(BF)
    out_ref[...] = jnp.broadcast_to(block[None], out_ref.shape)


def attend(samples, width_of_rows):
    scale = HD ** (-0.5)
    shape = (samples[0][0].shape[0], width_of_rows)
    column = lax.broadcasted_iota(jnp.int32, shape, 1)
    on_key = column % 2 == 0
    limit = jnp.where(on_key, -1, column)
    row = lax.broadcasted_iota(jnp.int32, (shape[0], 1), 0)
    contract_last = (((1,), (1,)), ((), ()))
    raw = []
    for queries, prompt, suffix, _, _, waits in samples:
        for wait in waits:
            wait()
        narrow = queries.astype(BF)
        raw.append(
            tuple(
                lax.dot_general(narrow, rows, contract_last, preferred_element_type=F32)
                for rows in (prompt(), suffix())
            )
        )
    held = []
    for (queries, _, _, width, pairs, _), (on_prompt, on_suffix) in zip(samples, raw):
        scores = jnp.where(on_key, on_prompt, pltpu.roll(on_suffix, 1, 1)) * scale
        scores = jnp.where(limit < width, scores, -1e30)
        singles = []
        for pair, since in pairs:
            score = jnp.sum(queries * pair[0:1], axis=1, keepdims=True) * scale
            singles.append(jnp.where(row >= since, score, -1e30) if since else score)
        highest = jnp.max(scores, axis=1, keepdims=True)
        for score in singles:
            highest = jnp.maximum(highest, score)
        spread = jnp.exp(scores - highest)
        single_spreads = [jnp.exp(score - highest) for score in singles]
        share = 1.0 / (jnp.sum(spread, axis=1, keepdims=True) + sum(single_spreads))
        weights = spread * share
        held.append(
            (
                jnp.where(on_key, 0.0, pltpu.roll(weights, 1, 1)).astype(BF),
                jnp.where(on_key, 0.0, weights).astype(BF),
                [(spread * share).astype(BF).astype(F32) for spread in single_spreads],
            )
        )
    results = []
    for (_, prompt, suffix, _, pairs, _), (prompt_weights, suffix_weights, single_weights) in zip(
        samples, held
    ):
        mixed = lax.dot(prompt_weights, prompt(), preferred_element_type=F32)
        mixed += lax.dot(suffix_weights, suffix(), preferred_element_type=F32)
        for (pair, _), weight in zip(pairs, single_weights):
            mixed += weight * pair[1:2]
        results.append(mixed.astype(BF))
    return results


def stay_kernel(*refs):
    far_prompt_ref, far_suffix_ref, *far_refs = refs[:9]
    rows_ref, pair_ref, prompt_ref, suffix_ref, facts_ref = refs[9:14]
    queries_ref, *near_refs, sems = refs[14:]
    slots = suffix_ref.shape[0]
    prompt_copy = pltpu.make_async_copy(far_prompt_ref, prompt_ref, sems.at[slots])
    suffix_copies = [
        pltpu.make_async_copy(far_suffix_ref.at[s], suffix_ref.at[s], sems.at[s])
        for s in range(slots)
    ]
    small_copies = [
        pltpu.make_async_copy(far, close, sems.at[slots + 1 + k])
        for k, (far, close) in enumerate(zip(far_refs, near_refs))
    ]
    for copy in (*small_copies, prompt_copy, *suffix_copies):
        copy.start()
    own = lax.axis_index("grp")
    for copy in small_copies:
        copy.wait()
    len_ref, slot_ref, moves_ref = near_refs[:3]
    query_first_ref, query_second_ref, fresh_first_ref, fresh_second_ref = near_refs[3:]
    is_source, (out_slot, destination) = look_up(moves_ref, own, 0, (1, 2))
    is_target, (in_source,) = look_up(moves_ref, own, 2, (0,))
    facts = (
        destination,
        2 * len_ref[own * slots + out_slot],
        out_slot,
        jnp.maximum(slot_ref[out_slot], 0),
        in_source,
        jnp.where(is_target == 1, slots + empty_slot_of(slot_ref), -1),
    )
    lane = lax.broadcasted_iota(jnp.int32, facts_ref.shape, 1)
    held = jnp.zeros(facts_ref.shape, jnp.int32)
    for k, value in enumerate(facts):
        held = jnp.where(lane == k, value, held)
    facts_ref[...] = held.astype(F32)
    for h in range(HEADS):
        queries_ref[:, h, :] = query_first_ref[:, h * HD : (h + 1) * HD].astype(F32)
        queries_ref[:, HEADS + h, :] = query_second_ref[:, h * HD : (h + 1) * HD].astype(F32)
    pair_ref[...] = fresh_first_ref[out_slot].astype(F32)
    mixed = attend(
        [
            (
                queries_ref[s],
                functools.partial(prompt_ref.__getitem__, jnp.maximum(slot_ref[s], 0)),
                functools.partial(suffix_ref.__getitem__, s),
                2 * len_ref[own * slots + s],
                ((fresh_first_ref[s].astype(F32), 0), (fresh_second_ref[s].astype(F32), HEADS)),
                [suffix_copies[s].wait] if s else [prompt_copy.wait, suffix_copies[0].wait],
            )
            for s in range(slots)
        ],
        suffix_ref.shape[1],
    )
    for s in range(slots):
        live = slot_ref[s] >= 0
        stays = live & jnp.logical_not((is_source == 1) & (out_slot == s))
        row = mixed[s].astype(F32)
        rows_ref[:, s, :] = jnp.where(live, row[:HEADS], 0.0)
        rows_ref[:, slots + s, :] = jnp.where(stays, row[HEADS:], 0.0)


def leave_kernel(facts_ref, offers_ref, prompt_ref, suffix_ref, pair_ref, moved_ref):
    offer = offers_ref[fact(facts_ref, 0)].astype(F32)
    half = HEADS // 2
    queries = jnp.concatenate(
        [
            offer[h // half : h // half + 1, h % half * HD : (h % half + 1) * HD]
            for h in range(HEADS)
        ],
        axis=0,
    )
    (mixed,) = attend(
        [
            (
                queries,
                functools.partial(prompt_ref.__getitem__, fact(facts_ref, 3)),
                functools.partial(suffix_ref.__getitem__, fact(facts_ref, 2)),
                fact(facts_ref, 1),
                ((pair_ref[...], 0), (offer[:, half * HD :], 0)),
                [],
            )
        ],
        suffix_ref.shape[1],
    )
    moved_ref[...] = jnp.broadcast_to(mixed[None], moved_ref.shape)


def merge_kernel(facts_ref, rows_ref, arrived_ref, out_ref):
    arrived = arrived_ref[fact(facts_ref, 4)].astype(F32)
    into = lax.broadcasted_iota(jnp.int32, rows_ref.shape[1:], 0) == fact(facts_ref, 5)
    for h in range(HEADS):
        row = jnp.where(into, arrived[h : h + 1], rows_ref[h])
        out_ref[:, h * HD : (h + 1) * HD] = row.astype(BF)


def sum_kernel(parts_ref, first_ref, second_ref):
    total = jnp.sum(parts_ref[...], axis=0)
    slots = first_ref.shape[0]
    first_ref[...] = total[:slots].astype(BF)
    second_ref[...] = total[slots:].astype(BF)


def per_device(
    suffix_cache,
    prompt_cache,
    query_first,
    fresh_first,
    query_second,
    fresh_second,
    out_weight,
    suffix_len,
    prompt_slot,
    moves,
):
    slots, cap = suffix_cache.shape[:2]
    prompts, prompt_len = prompt_cache.shape[:2]
    groups = lax.axis_size("grp")
    shares = lax.axis_size("tp")
    features = out_weight.shape[1]
    suffix_rows = suffix_cache.reshape(slots, 2 * cap, HD)
    prompt_rows = prompt_cache.reshape(prompts, 2 * prompt_len, HD)
    offer = pl.pallas_call(
        offer_kernel,
        out_shape=pltpu.VMEM((groups, 2, (HEADS // 2 + 1) * HD), BF),
        in_specs=[SMEM, VMEM, VMEM],
        out_specs=VMEM,
        name="offer",
    )(prompt_slot, query_second, fresh_second)
    offers = lax.all_to_all(offer, "grp", 0, 0, tiled=True)
    tables = (suffix_len, prompt_slot, moves)
    vectors = (query_first, query_second, fresh_first, fresh_second)
    rows, pair, near_prompt, near_suffix, facts = pl.pallas_call(
        stay_kernel,
        out_shape=(
            pltpu.VMEM((HEADS, 2 * slots, HD), F32),
            pltpu.VMEM((2, HD), F32),
            pltpu.VMEM(prompt_rows.shape, BF),
            pltpu.VMEM(suffix_rows.shape, BF),
            pltpu.VMEM((1, HD), F32),
        ),
        in_specs=[ANY] * 9,
        out_specs=(VMEM,) * 5,
        scratch_shapes=[
            pltpu.VMEM((slots, 2 * HEADS, HD), F32),
            *(pltpu.SMEM(table.shape, jnp.int32) for table in tables),
            *(pltpu.VMEM(array.shape, BF) for array in vectors),
            pltpu.SemaphoreType.DMA((slots + 1 + len(tables) + len(vectors),)),
        ],
        name="stay",
    )(prompt_rows, suffix_rows, *tables, *vectors)
    moved = pl.pallas_call(
        leave_kernel,
        out_shape=pltpu.VMEM((groups, HEADS, HD), BF),
        in_specs=[VMEM] * 5,
        out_specs=VMEM,
        compiler_params=SMALL,
        cost_estimate=pl.CostEstimate(flops=10**11, transcendentals=0, bytes_accessed=1 << 20),
        name="leave",
    )(near(facts), near(offers), near(near_prompt), near(near_suffix), near(pair))
    arrived = lax.all_to_all(moved, "grp", 0, 0, tiled=True)
    merged = pl.pallas_call(
        merge_kernel,
        out_shape=pltpu.VMEM((2 * slots, HEADS * HD), BF),
        in_specs=[VMEM] * 3,
        out_specs=VMEM,
        compiler_params=SMALL,
        name="merge",
    )(near(facts), near(rows), near(arrived))
    parts = jnp.dot(merged, out_weight, preferred_element_type=F32)
    parts = parts.reshape(2 * slots, shares, features // shares).swapaxes(0, 1)
    parts = lax.all_to_all(parts, "tp", 0, 0, tiled=True)
    out = jax.ShapeDtypeStruct((slots, features // shares), BF)
    return pl.pallas_call(
        sum_kernel,
        out_shape=(out, out),
        in_specs=[VMEM],
        out_specs=(VMEM, VMEM),
        compiler_params=SMALL,
        name="sum",
    )(near(parts))


def solution(mesh):
    placed = (
        P("grp", None, None, "tp"),
        P("grp", None, None, "tp"),
        P("grp", "tp"),
        P("grp", None, "tp"),
        P("grp", "tp"),
        P("grp", None, "tp"),
        P("tp", None),
        P(),
        P("grp"),
        P(),
    )
    return jax.shard_map(
        per_device,
        mesh=mesh,
        in_specs=placed,
        out_specs=(P("grp", "tp"), P("grp", "tp")),
        check_vma=False,
    )
```

```python
import functools

import jax
import jax.numpy as jnp
from jax import lax
from jax.experimental import pallas as pl
from jax.experimental.pallas import tpu as pltpu
from jax.sharding import PartitionSpec as P

QH = 64
KVH = 8
HD = 128
HEADS = QH // KVH

BF = jnp.bfloat16
F32 = jnp.float32
SMEM = pl.BlockSpec(memory_space=pltpu.SMEM)
VMEM = pl.BlockSpec(memory_space=pltpu.VMEM)
ANY = pl.BlockSpec(memory_space=pl.ANY)


SMALL = pltpu.CompilerParams(vmem_limit_bytes=8 << 20)


def near(array):
    return pltpu.with_memory_space_constraint(array, pltpu.VMEM)


def empty_slot_of(slot_ref):
    found = jnp.int32(0)
    for s in range(slot_ref.shape[0]):
        found = jnp.where(slot_ref[s] < 0, jnp.int32(s), found)
    return found


def look_up(moves_ref, own, key, fields):
    hit_any = jnp.int32(0)
    values = [jnp.int32(0) for _ in fields]
    for i in range(moves_ref.shape[0]):
        hit = moves_ref[i, key] == own
        hit_any = jnp.where(hit, jnp.int32(1), hit_any)
        values = [jnp.where(hit, moves_ref[i, f], v) for f, v in zip(fields, values)]
    return hit_any, values


def fact(facts_ref, k):
    lane = lax.broadcasted_iota(jnp.int32, facts_ref.shape, 1)
    return jnp.sum(jnp.where(lane == k, facts_ref[...], 0.0)).astype(jnp.int32)


def offer_kernel(slot_ref, query_ref, fresh_ref, out_ref):
    empty = empty_slot_of(slot_ref)
    slots = query_ref.shape[0]
    half = query_ref.shape[1] // 2
    mine = lax.broadcasted_iota(jnp.int32, (slots, half), 0) == empty
    pair = jnp.zeros((2, HD), F32)
    for s in range(slots):
        pair = jnp.where(empty == s, fresh_ref[s].astype(F32), pair)
    rows = []
    for r in range(2):
        part = query_ref[:, r * half : (r + 1) * half].astype(F32)
        heads = jnp.sum(jnp.where(mine, part, 0.0), axis=0, keepdims=True)
        rows.append(jnp.concatenate([heads, pair[r : r + 1]], axis=1))
    block = jnp.concatenate(rows, axis=0).astype(BF)
    out_ref[...] = jnp.broadcast_to(block[None], out_ref.shape)


def attend(samples, width_of_rows):
    scale = HD ** (-0.5)
    shape = (samples[0][0].shape[0], width_of_rows)
    column = lax.broadcasted_iota(jnp.int32, shape, 1)
    on_key = column % 2 == 0
    limit = jnp.where(on_key, -1, column)
    row = lax.broadcasted_iota(jnp.int32, (shape[0], 1), 0)
    contract_last = (((1,), (1,)), ((), ()))
    raw = []
    for queries, prompt, suffix, _, _, waits in samples:
        for wait in waits:
            wait()
        narrow = queries.astype(BF)
        raw.append(
            tuple(
                lax.dot_general(narrow, rows, contract_last, preferred_element_type=F32)
                for rows in (prompt(), suffix())
            )
        )
    held = []
    for (queries, _, _, width, pairs, _), (on_prompt, on_suffix) in zip(samples, raw):
        scores = jnp.where(on_key, on_prompt, pltpu.roll(on_suffix, 1, 1)) * scale
        scores = jnp.where(limit < width, scores, -1e30)
        singles = []
        for pair, since in pairs:
            score = jnp.sum(queries * pair[0:1], axis=1, keepdims=True) * scale
            singles.append(jnp.where(row >= since, score, -1e30) if since else score)
        highest = jnp.max(scores, axis=1, keepdims=True)
        for score in singles:
            highest = jnp.maximum(highest, score)
        spread = jnp.exp(scores - highest)
        single_spreads = [jnp.exp(score - highest) for score in singles]
        share = 1.0 / (jnp.sum(spread, axis=1, keepdims=True) + sum(single_spreads))
        weights = spread * share
        held.append(
            (
                jnp.where(on_key, 0.0, pltpu.roll(weights, 1, 1)).astype(BF),
                jnp.where(on_key, 0.0, weights).astype(BF),
                [(spread * share).astype(BF).astype(F32) for spread in single_spreads],
            )
        )
    results = []
    for (_, prompt, suffix, _, pairs, _), (prompt_weights, suffix_weights, single_weights) in zip(
        samples, held
    ):
        mixed = lax.dot(prompt_weights, prompt(), preferred_element_type=F32)
        mixed += lax.dot(suffix_weights, suffix(), preferred_element_type=F32)
        for (pair, _), weight in zip(pairs, single_weights):
            mixed += weight * pair[1:2]
        results.append(mixed.astype(BF))
    return results


def stay_kernel(*refs):
    far_prompt_ref, far_suffix_ref, *far_refs = refs[:9]
    rows_ref, pair_ref, prompt_ref, suffix_ref, facts_ref = refs[9:14]
    queries_ref, *near_refs, sems = refs[14:]
    slots = suffix_ref.shape[0]
    prompt_copy = pltpu.make_async_copy(far_prompt_ref, prompt_ref, sems.at[slots])
    suffix_copies = [
        pltpu.make_async_copy(far_suffix_ref.at[s], suffix_ref.at[s], sems.at[s])
        for s in range(slots)
    ]
    small_copies = [
        pltpu.make_async_copy(far, close, sems.at[slots + 1 + k])
        for k, (far, close) in enumerate(zip(far_refs, near_refs))
    ]
    for copy in (*small_copies, prompt_copy, *suffix_copies):
        copy.start()
    own = lax.axis_index("grp")
    for copy in small_copies:
        copy.wait()
    len_ref, slot_ref, moves_ref = near_refs[:3]
    query_first_ref, query_second_ref, fresh_first_ref, fresh_second_ref = near_refs[3:]
    is_source, (out_slot, destination) = look_up(moves_ref, own, 0, (1, 2))
    is_target, (in_source,) = look_up(moves_ref, own, 2, (0,))
    facts = (
        destination,
        2 * len_ref[own * slots + out_slot],
        out_slot,
        jnp.maximum(slot_ref[out_slot], 0),
        in_source,
        jnp.where(is_target == 1, slots + empty_slot_of(slot_ref), -1),
    )
    lane = lax.broadcasted_iota(jnp.int32, facts_ref.shape, 1)
    held = jnp.zeros(facts_ref.shape, jnp.int32)
    for k, value in enumerate(facts):
        held = jnp.where(lane == k, value, held)
    facts_ref[...] = held.astype(F32)
    for h in range(HEADS):
        queries_ref[:, h, :] = query_first_ref[:, h * HD : (h + 1) * HD].astype(F32)
        queries_ref[:, HEADS + h, :] = query_second_ref[:, h * HD : (h + 1) * HD].astype(F32)
    pair_ref[...] = fresh_first_ref[out_slot].astype(F32)
    mixed = attend(
        [
            (
                queries_ref[s],
                functools.partial(prompt_ref.__getitem__, jnp.maximum(slot_ref[s], 0)),
                functools.partial(suffix_ref.__getitem__, s),
                2 * len_ref[own * slots + s],
                ((fresh_first_ref[s].astype(F32), 0), (fresh_second_ref[s].astype(F32), HEADS)),
                [suffix_copies[s].wait] if s else [prompt_copy.wait, suffix_copies[0].wait],
            )
            for s in range(slots)
        ],
        suffix_ref.shape[1],
    )
    for s in range(slots):
        live = slot_ref[s] >= 0
        stays = live & jnp.logical_not((is_source == 1) & (out_slot == s))
        row = mixed[s].astype(F32)
        rows_ref[:, s, :] = jnp.where(live, row[:HEADS], 0.0)
        rows_ref[:, slots + s, :] = jnp.where(stays, row[HEADS:], 0.0)


def leave_kernel(facts_ref, offers_ref, prompt_ref, suffix_ref, pair_ref, moved_ref):
    offer = offers_ref[fact(facts_ref, 0)].astype(F32)
    half = HEADS // 2
    queries = jnp.concatenate(
        [
            offer[h // half : h // half + 1, h % half * HD : (h % half + 1) * HD]
            for h in range(HEADS)
        ],
        axis=0,
    )
    (mixed,) = attend(
        [
            (
                queries,
                functools.partial(prompt_ref.__getitem__, fact(facts_ref, 3)),
                functools.partial(suffix_ref.__getitem__, fact(facts_ref, 2)),
                fact(facts_ref, 1),
                ((pair_ref[...], 0), (offer[:, half * HD :], 0)),
                [],
            )
        ],
        suffix_ref.shape[1],
    )
    moved_ref[...] = jnp.broadcast_to(mixed[None], moved_ref.shape)


def merge_kernel(facts_ref, rows_ref, arrived_ref, out_ref):
    arrived = arrived_ref[fact(facts_ref, 4)].astype(F32)
    into = lax.broadcasted_iota(jnp.int32, rows_ref.shape[1:], 0) == fact(facts_ref, 5)
    for h in range(HEADS):
        row = jnp.where(into, arrived[h : h + 1], rows_ref[h])
        out_ref[:, h * HD : (h + 1) * HD] = row.astype(BF)


def sum_kernel(parts_ref, first_ref, second_ref):
    total = jnp.sum(parts_ref[...].astype(F32), axis=0)
    slots = first_ref.shape[0]
    first_ref[...] = total[:slots].astype(BF)
    second_ref[...] = total[slots:].astype(BF)


def per_device(
    suffix_cache,
    prompt_cache,
    query_first,
    fresh_first,
    query_second,
    fresh_second,
    out_weight,
    suffix_len,
    prompt_slot,
    moves,
):
    slots, cap = suffix_cache.shape[:2]
    prompts, prompt_len = prompt_cache.shape[:2]
    groups = lax.axis_size("grp")
    shares = lax.axis_size("tp")
    features = out_weight.shape[1]
    suffix_rows = suffix_cache.reshape(slots, 2 * cap, HD)
    prompt_rows = prompt_cache.reshape(prompts, 2 * prompt_len, HD)
    offer = pl.pallas_call(
        offer_kernel,
        out_shape=pltpu.VMEM((groups, 2, (HEADS // 2 + 1) * HD), BF),
        in_specs=[SMEM, VMEM, VMEM],
        out_specs=VMEM,
        name="offer",
    )(prompt_slot, query_second, fresh_second)
    offers = lax.all_to_all(offer, "grp", 0, 0, tiled=True)
    tables = (suffix_len, prompt_slot, moves)
    vectors = (query_first, query_second, fresh_first, fresh_second)
    rows, pair, near_prompt, near_suffix, facts = pl.pallas_call(
        stay_kernel,
        out_shape=(
            pltpu.VMEM((HEADS, 2 * slots, HD), F32),
            pltpu.VMEM((2, HD), F32),
            pltpu.VMEM(prompt_rows.shape, BF),
            pltpu.VMEM(suffix_rows.shape, BF),
            pltpu.VMEM((1, HD), F32),
        ),
        in_specs=[ANY] * 9,
        out_specs=(VMEM,) * 5,
        scratch_shapes=[
            pltpu.VMEM((slots, 2 * HEADS, HD), F32),
            *(pltpu.SMEM(table.shape, jnp.int32) for table in tables),
            *(pltpu.VMEM(array.shape, BF) for array in vectors),
            pltpu.SemaphoreType.DMA((slots + 1 + len(tables) + len(vectors),)),
        ],
        name="stay",
    )(prompt_rows, suffix_rows, *tables, *vectors)
    moved = pl.pallas_call(
        leave_kernel,
        out_shape=pltpu.VMEM((groups, HEADS, HD), BF),
        in_specs=[VMEM] * 5,
        out_specs=VMEM,
        compiler_params=SMALL,
        cost_estimate=pl.CostEstimate(flops=10**11, transcendentals=0, bytes_accessed=1 << 20),
        name="leave",
    )(near(facts), near(offers), near(near_prompt), near(near_suffix), near(pair))
    arrived = lax.all_to_all(moved, "grp", 0, 0, tiled=True)
    merged = pl.pallas_call(
        merge_kernel,
        out_shape=pltpu.VMEM((2 * slots, HEADS * HD), BF),
        in_specs=[VMEM] * 3,
        out_specs=VMEM,
        compiler_params=SMALL,
        name="merge",
    )(near(facts), near(rows), near(arrived))
    parts = jnp.dot(merged, out_weight, preferred_element_type=F32).astype(BF)
    parts = parts.reshape(2 * slots, shares, features // shares).swapaxes(0, 1)
    parts = lax.all_to_all(parts, "tp", 0, 0, tiled=True)
    out = jax.ShapeDtypeStruct((slots, features // shares), BF)
    return pl.pallas_call(
        sum_kernel,
        out_shape=(out, out),
        in_specs=[VMEM],
        out_specs=(VMEM, VMEM),
        compiler_params=SMALL,
        name="sum",
    )(near(parts))


def solution(mesh):
    placed = (
        P("grp", None, None, "tp"),
        P("grp", None, None, "tp"),
        P("grp", "tp"),
        P("grp", None, "tp"),
        P("grp", "tp"),
        P("grp", None, "tp"),
        P("tp", None),
        P(),
        P("grp"),
        P(),
    )
    return jax.shard_map(
        per_device,
        mesh=mesh,
        in_specs=placed,
        out_specs=(P("grp", "tp"), P("grp", "tp")),
        check_vma=False,
    )
```

```python
import functools

import jax
import jax.numpy as jnp
from jax import lax
from jax.experimental import pallas as pl
from jax.experimental.pallas import tpu as pltpu
from jax.sharding import PartitionSpec as P

QH = 64
KVH = 8
HD = 128
HEADS = QH // KVH

BF = jnp.bfloat16
F32 = jnp.float32
SMEM = pl.BlockSpec(memory_space=pltpu.SMEM)
VMEM = pl.BlockSpec(memory_space=pltpu.VMEM)
ANY = pl.BlockSpec(memory_space=pl.ANY)


SMALL = pltpu.CompilerParams(vmem_limit_bytes=8 << 20)


def near(array):
    return pltpu.with_memory_space_constraint(array, pltpu.VMEM)


def empty_slot_of(slot_ref):
    found = jnp.int32(0)
    for s in range(slot_ref.shape[0]):
        found = jnp.where(slot_ref[s] < 0, jnp.int32(s), found)
    return found


def look_up(moves_ref, own, key, fields):
    hit_any = jnp.int32(0)
    values = [jnp.int32(0) for _ in fields]
    for i in range(moves_ref.shape[0]):
        hit = moves_ref[i, key] == own
        hit_any = jnp.where(hit, jnp.int32(1), hit_any)
        values = [jnp.where(hit, moves_ref[i, f], v) for f, v in zip(fields, values)]
    return hit_any, values


def fact(facts_ref, k):
    lane = lax.broadcasted_iota(jnp.int32, facts_ref.shape, 1)
    return jnp.sum(jnp.where(lane == k, facts_ref[...], 0.0)).astype(jnp.int32)


def offer_kernel(slot_ref, query_ref, fresh_ref, out_ref):
    empty = empty_slot_of(slot_ref)
    slots = query_ref.shape[0]
    half = query_ref.shape[1] // 2
    mine = lax.broadcasted_iota(jnp.int32, (slots, half), 0) == empty
    pair = jnp.zeros((2, HD), F32)
    for s in range(slots):
        pair = jnp.where(empty == s, fresh_ref[s].astype(F32), pair)
    rows = []
    for r in range(2):
        part = query_ref[:, r * half : (r + 1) * half].astype(F32)
        heads = jnp.sum(jnp.where(mine, part, 0.0), axis=0, keepdims=True)
        rows.append(jnp.concatenate([heads, pair[r : r + 1]], axis=1))
    block = jnp.concatenate(rows, axis=0).astype(BF)
    out_ref[...] = jnp.broadcast_to(block[None], out_ref.shape)


def attend(samples, width_of_rows):
    scale = HD ** (-0.5)
    shape = (samples[0][0].shape[0], width_of_rows)
    column = lax.broadcasted_iota(jnp.int32, shape, 1)
    on_key = column % 2 == 0
    limit = jnp.where(on_key, -1, column)
    row = lax.broadcasted_iota(jnp.int32, (shape[0], 1), 0)
    contract_last = (((1,), (1,)), ((), ()))
    raw = []
    for queries, prompt, suffix, _, _, waits in samples:
        for wait in waits:
            wait()
        narrow = queries.astype(BF)
        raw.append(
            tuple(
                lax.dot_general(narrow, rows, contract_last, preferred_element_type=F32)
                for rows in (prompt(), suffix())
            )
        )
    held = []
    for (queries, _, _, width, pairs, _), (on_prompt, on_suffix) in zip(samples, raw):
        scores = jnp.where(on_key, on_prompt, pltpu.roll(on_suffix, 1, 1)) * scale
        scores = jnp.where(limit < width, scores, -1e30)
        singles = []
        for pair, since in pairs:
            score = jnp.sum(queries * pair[0:1], axis=1, keepdims=True) * scale
            singles.append(jnp.where(row >= since, score, -1e30) if since else score)
        highest = jnp.max(scores, axis=1, keepdims=True)
        for score in singles:
            highest = jnp.maximum(highest, score)
        spread = jnp.exp(scores - highest)
        single_spreads = [jnp.exp(score - highest) for score in singles]
        share = 1.0 / (jnp.sum(spread, axis=1, keepdims=True) + sum(single_spreads))
        weights = spread * share
        held.append(
            (
                jnp.where(on_key, 0.0, pltpu.roll(weights, 1, 1)).astype(BF),
                jnp.where(on_key, 0.0, weights).astype(BF),
                [(spread * share).astype(BF).astype(F32) for spread in single_spreads],
            )
        )
    results = []
    for (_, prompt, suffix, _, pairs, _), (prompt_weights, suffix_weights, single_weights) in zip(
        samples, held
    ):
        mixed = lax.dot(prompt_weights, prompt(), preferred_element_type=F32)
        mixed += lax.dot(suffix_weights, suffix(), preferred_element_type=F32)
        for (pair, _), weight in zip(pairs, single_weights):
            mixed += weight * pair[1:2]
        results.append(mixed.astype(BF))
    return results


def stay_kernel(*refs):
    far_prompt_ref, far_suffix_ref, *far_refs = refs[:9]
    rows_ref, pair_ref, kept_ref, facts_ref = refs[9:13]
    prompt_ref, suffix_ref, queries_ref, *near_refs, sems = refs[13:]
    slots = suffix_ref.shape[0]
    prompt_copy = pltpu.make_async_copy(far_prompt_ref, prompt_ref, sems.at[slots])
    suffix_copies = [
        pltpu.make_async_copy(far_suffix_ref.at[s], suffix_ref.at[s], sems.at[s])
        for s in range(slots)
    ]
    small_copies = [
        pltpu.make_async_copy(far, close, sems.at[slots + 1 + k])
        for k, (far, close) in enumerate(zip(far_refs, near_refs))
    ]
    for copy in (*small_copies, prompt_copy, *suffix_copies):
        copy.start()
    own = lax.axis_index("grp")
    for copy in small_copies:
        copy.wait()
    len_ref, slot_ref, moves_ref = near_refs[:3]
    query_first_ref, query_second_ref, fresh_first_ref, fresh_second_ref = near_refs[3:]
    is_source, (out_slot, destination) = look_up(moves_ref, own, 0, (1, 2))
    is_target, (in_source,) = look_up(moves_ref, own, 2, (0,))
    last = slots + 1 + len(small_copies)
    own_prompt = far_prompt_ref.at[jnp.maximum(slot_ref[out_slot], 0)]
    kept_copies = (
        pltpu.make_async_copy(own_prompt, kept_ref.at[0], sems.at[last]),
        pltpu.make_async_copy(far_suffix_ref.at[out_slot], kept_ref.at[1], sems.at[last + 1]),
    )
    for copy in kept_copies:
        copy.start()
    facts = (
        destination,
        2 * len_ref[own * slots + out_slot],
        in_source,
        jnp.where(is_target == 1, slots + empty_slot_of(slot_ref), -1),
    )
    lane = lax.broadcasted_iota(jnp.int32, facts_ref.shape, 1)
    held = jnp.zeros(facts_ref.shape, jnp.int32)
    for k, value in enumerate(facts):
        held = jnp.where(lane == k, value, held)
    facts_ref[...] = held.astype(F32)
    for h in range(HEADS):
        queries_ref[:, h, :] = query_first_ref[:, h * HD : (h + 1) * HD].astype(F32)
        queries_ref[:, HEADS + h, :] = query_second_ref[:, h * HD : (h + 1) * HD].astype(F32)
    pair_ref[...] = fresh_first_ref[out_slot].astype(F32)
    mixed = attend(
        [
            (
                queries_ref[s],
                functools.partial(prompt_ref.__getitem__, jnp.maximum(slot_ref[s], 0)),
                functools.partial(suffix_ref.__getitem__, s),
                2 * len_ref[own * slots + s],
                ((fresh_first_ref[s].astype(F32), 0), (fresh_second_ref[s].astype(F32), HEADS)),
                [suffix_copies[s].wait] if s else [prompt_copy.wait, suffix_copies[0].wait],
            )
            for s in range(slots)
        ],
        suffix_ref.shape[1],
    )
    for s in range(slots):
        live = slot_ref[s] >= 0
        stays = live & jnp.logical_not((is_source == 1) & (out_slot == s))
        row = mixed[s].astype(F32)
        rows_ref[:, s, :] = jnp.where(live, row[:HEADS], 0.0)
        rows_ref[:, slots + s, :] = jnp.where(stays, row[HEADS:], 0.0)
    for copy in kept_copies:
        copy.wait()


def leave_kernel(facts_ref, offers_ref, kept_ref, pair_ref, moved_ref):
    offer = offers_ref[fact(facts_ref, 0)].astype(F32)
    half = HEADS // 2
    queries = jnp.concatenate(
        [
            offer[h // half : h // half + 1, h % half * HD : (h % half + 1) * HD]
            for h in range(HEADS)
        ],
        axis=0,
    )
    (mixed,) = attend(
        [
            (
                queries,
                functools.partial(kept_ref.__getitem__, 0),
                functools.partial(kept_ref.__getitem__, 1),
                fact(facts_ref, 1),
                ((pair_ref[...], 0), (offer[:, half * HD :], 0)),
                [],
            )
        ],
        kept_ref.shape[1],
    )
    moved_ref[...] = jnp.broadcast_to(mixed[None], moved_ref.shape)


def merge_kernel(facts_ref, rows_ref, arrived_ref, out_ref):
    arrived = arrived_ref[fact(facts_ref, 2)].astype(F32)
    into = lax.broadcasted_iota(jnp.int32, rows_ref.shape[1:], 0) == fact(facts_ref, 3)
    for h in range(HEADS):
        row = jnp.where(into, arrived[h : h + 1], rows_ref[h])
        out_ref[:, h * HD : (h + 1) * HD] = row.astype(BF)


def sum_kernel(parts_ref, first_ref, second_ref):
    total = jnp.sum(parts_ref[...].astype(F32), axis=0)
    slots = first_ref.shape[0]
    first_ref[...] = total[:slots].astype(BF)
    second_ref[...] = total[slots:].astype(BF)


def per_device(
    suffix_cache,
    prompt_cache,
    query_first,
    fresh_first,
    query_second,
    fresh_second,
    out_weight,
    suffix_len,
    prompt_slot,
    moves,
):
    slots, cap = suffix_cache.shape[:2]
    prompts, prompt_len = prompt_cache.shape[:2]
    groups = lax.axis_size("grp")
    shares = lax.axis_size("tp")
    features = out_weight.shape[1]
    suffix_rows = suffix_cache.reshape(slots, 2 * cap, HD)
    prompt_rows = prompt_cache.reshape(prompts, 2 * prompt_len, HD)
    offer = pl.pallas_call(
        offer_kernel,
        out_shape=pltpu.VMEM((groups, 2, (HEADS // 2 + 1) * HD), BF),
        in_specs=[SMEM, VMEM, VMEM],
        out_specs=VMEM,
        name="offer",
    )(prompt_slot, query_second, fresh_second)
    offers = lax.all_to_all(offer, "grp", 0, 0, tiled=True)
    tables = (suffix_len, prompt_slot, moves)
    vectors = (query_first, query_second, fresh_first, fresh_second)
    rows, pair, kept, facts = pl.pallas_call(
        stay_kernel,
        out_shape=(
            pltpu.VMEM((HEADS, 2 * slots, HD), F32),
            pltpu.VMEM((2, HD), F32),
            pltpu.VMEM((2, *suffix_rows.shape[1:]), BF),
            pltpu.VMEM((1, HD), F32),
        ),
        in_specs=[ANY] * 9,
        out_specs=(VMEM,) * 4,
        scratch_shapes=[
            pltpu.VMEM(prompt_rows.shape, BF),
            pltpu.VMEM(suffix_rows.shape, BF),
            pltpu.VMEM((slots, 2 * HEADS, HD), F32),
            *(pltpu.SMEM(table.shape, jnp.int32) for table in tables),
            *(pltpu.VMEM(array.shape, BF) for array in vectors),
            pltpu.SemaphoreType.DMA((slots + 3 + len(tables) + len(vectors),)),
        ],
        name="stay",
    )(prompt_rows, suffix_rows, *tables, *vectors)
    moved = pl.pallas_call(
        leave_kernel,
        out_shape=pltpu.VMEM((groups, HEADS, HD), BF),
        in_specs=[VMEM] * 4,
        out_specs=VMEM,
        compiler_params=SMALL,
        cost_estimate=pl.CostEstimate(flops=10**11, transcendentals=0, bytes_accessed=1 << 20),
        name="leave",
    )(near(facts), near(offers), near(kept), near(pair))
    arrived = lax.all_to_all(moved, "grp", 0, 0, tiled=True)
    merged = pl.pallas_call(
        merge_kernel,
        out_shape=pltpu.VMEM((2 * slots, HEADS * HD), BF),
        in_specs=[VMEM] * 3,
        out_specs=VMEM,
        compiler_params=SMALL,
        name="merge",
    )(near(facts), near(rows), near(arrived))
    parts = jnp.dot(merged, out_weight, preferred_element_type=F32).astype(BF)
    parts = parts.reshape(2 * slots, shares, features // shares).swapaxes(0, 1)
    parts = lax.all_to_all(parts, "tp", 0, 0, tiled=True)
    out = jax.ShapeDtypeStruct((slots, features // shares), BF)
    return pl.pallas_call(
        sum_kernel,
        out_shape=(out, out),
        in_specs=[VMEM],
        out_specs=(VMEM, VMEM),
        compiler_params=SMALL,
        name="sum",
    )(near(parts))


def solution(mesh):
    placed = (
        P("grp", None, None, "tp"),
        P("grp", None, None, "tp"),
        P("grp", "tp"),
        P("grp", None, "tp"),
        P("grp", "tp"),
        P("grp", None, "tp"),
        P("tp", None),
        P(),
        P("grp"),
        P(),
    )
    return jax.shard_map(
        per_device,
        mesh=mesh,
        in_specs=placed,
        out_specs=(P("grp", "tp"), P("grp", "tp")),
        check_vma=False,
    )
```
